128 devices in a mesh: rows: 8 (over z, y_hi), snaps: 16 (over x, y_lo, core).
Axes of the slice: x: 4, y: 4 (y_hi: 2, y_lo: 2; y = y_hi * 2 + y_lo), z: 4, core: 2. Of those that a mesh axis runs over, the one named last changes fastest.
Arguments:
- snapshots: float32 [16384, 4096], P('rows', 'snaps'), may hold values from -6 to 6
- weights: float32 [16384], P('rows'), may hold values from 0.3 to 3
- next_bricks: float32 [16384, 4096], P(('rows', 'snaps')), may hold values from -6 to 6
- brick_source: int32 [8, 64], P('rows'), may hold values from 0 to 63, each once within a row
Outputs:
- gram: float32 [4096, 4096], P('rows', 'snaps')
- next_tiles: float32 [16384, 4096], P('rows', 'snaps')
The draws below stay inside these ranges and needn't reach their ends.
Inputs may be any that keep to these rules, and one draw needn't show every extreme that they name: Each row of brick_source is a permutation of 0 to 63.
All inputs are finite; a program needn't handle non-finite values.
Results may differ from the reference program's by a relative error of at most 0.00007.
Values sent between devices are 32-bit elements; how exact they have to be, the bound alone decides.
A program may use at most 128 MiB of HBM per device.

```python
import math
import jax
import jax.numpy as jnp
from jax import lax

BRICK = 32
S = 4096
M = 16384
BRICKS_DEV = 64
N_ROWS = 8


def level_of(stream_key, extent, shards, low, high):
    factor_of = 1.0
    for position, parts in shards:
        heights = jax.random.uniform(jax.random.fold_in(jax.random.fold_in(stream_key, 6), position), (parts,), jnp.float32, low / len(shards), high / len(shards))
        factor_of = factor_of * jnp.repeat(jnp.exp(heights), extent[position] // parts).reshape((-1,) + (1,) * (len(extent) - 1 - position))
    return factor_of


def normal_values(stream_key, dims, scale, reach, pieces=(), dtype=jnp.bfloat16):
    result = jax.random.normal(stream_key, dims, jnp.float32) * scale
    if len(pieces) > 0:
        result = level_of(stream_key, dims, pieces, -0.22, 0.18) * result
    return jnp.clip(result, min=-reach, max=reach).astype(dtype)


def setup_inputs(seed: int = 0) -> dict:
    key_of = jax.random.split(jax.random.key(seed), 5)
    snapshots = normal_values(key_of[0], (M, S), 1.0, 6.0, ((0, 8), (1, 16)), jnp.float32)
    weights = jnp.clip(jnp.exp(math.log(3.0) - 2.3025851 * jax.random.uniform(key_of[1], (M,), jnp.float32) ** level_of(key_of[1], (M,), ((0, 8),), -0.2, 0.2)), 0.3, 3.0)
    next_bricks = normal_values(key_of[2], (M, S), 1.0, 6.0, ((0, 128),), jnp.float32)
    brick_source = jax.vmap(lambda own: jax.random.permutation(own, BRICKS_DEV))(jax.random.split(key_of[3], N_ROWS)).reshape((N_ROWS, BRICKS_DEV)).astype(jnp.int32)
    return dict(snapshots=snapshots, weights=weights, next_bricks=next_bricks, brick_source=brick_source)


def pick_bricks(block, order):
    return jnp.take(block, order, axis=0)

def reference(snapshots, weights, next_bricks, brick_source):
    weighted = snapshots * weights[:, None]
    product = lax.dot_general(snapshots, weighted, (((0,), (0,)), ((), ())), precision=lax.Precision.HIGHEST, preferred_element_type=jnp.float32)
    gram = product / jnp.float32(math.sqrt(M))
    blocks = next_bricks.reshape(N_ROWS, BRICKS_DEV, BRICK, S)
    moved = jax.vmap(pick_bricks)(blocks, brick_source)
    next_tiles = moved.reshape(M, S)
    return (gram, next_tiles)
```

```python
import functools
import math

import jax
import jax.numpy as jnp
from jax import lax
from jax.experimental import pallas as pl
from jax.experimental.pallas import tpu as pltpu
from jax.sharding import PartitionSpec as P

BRICK = 32
NX, NZ = 4, 4
CHUNKS = 8
LANES = 128
LAG = 5
MESH = pl.DeviceIdType.MESH


def kernel(
    scale, snap, w_ref, bricks, gram, landed,
    xs, ahi, alo, bhi, blo, ps, zp, zm, ys,
    sem_a, sem_x, sem_h, sem_s, sem_p, sem_m, sem_y, sem_b,
    out_a, out_x, out_h, out_s, out_p, out_m, out_y, out_b,
):
    rb, me = lax.axis_index("rows"), lax.axis_index("snaps")
    z, y_hi = rb // 2, rb % 2
    x, y_lo, c = me // 4, (me // 2) % 2, me % 2
    y = y_hi * 2 + y_lo
    quarter = y_lo * 2 + c
    depth = xs.shape[3]
    half = depth // 2

    def snap_of(xx, yl, cc):
        return xx * 4 + yl * 2 + cc

    right = (rb, snap_of((x + 1) % NX, y_lo, c))
    left = (rb, snap_of((x + 3) % NX, y_lo, c))
    twin = (rb, snap_of(x, y_lo, 1 - c))
    up = (((z + 1) % NZ) * 2 + y_hi, me)
    down = (((z + 3) % NZ) * 2 + y_hi, me)

    def send(src, dst, s_sem, r_sem, to):
        return pltpu.make_async_remote_copy(
            src_ref=src, dst_ref=dst, send_sem=s_sem, recv_sem=r_sem, device_id=to, device_id_type=MESH
        )

    def arrived(dst, sem):
        pltpu.make_async_copy(dst, dst, sem).wait()

    barrier = pltpu.get_barrier_semaphore()
    for o in range(1, 16):
        pl.semaphore_signal(barrier, inc=1, device_id=(rb, (me + o) % 16), device_id_type=MESH)
    pl.semaphore_signal(barrier, inc=1, device_id=up, device_id_type=MESH)
    pl.semaphore_signal(barrier, inc=1, device_id=down, device_id_type=MESH)
    for yl in range(2):
        far = (z * 2 + 1 - y_hi, snap_of(x, yl, c))
        pl.semaphore_signal(barrier, inc=1, device_id=far, device_id_type=MESH)
    pl.semaphore_wait(barrier, 19)

    def reshard(o, part):
        q2 = (quarter + o) % 4
        k = part * 4 + c * 2 + y_lo
        src = snap.at[pl.ds(pl.multiple_of(q2 * depth, depth), depth), pl.ds(part * LANES, LANES)]
        dst = xs.at[q2 % 2, 0, k]
        if o == 0:
            return pltpu.make_async_copy(src, dst, sem_a.at[k])
        to = (rb, snap_of(x, q2 // 2, q2 % 2))
        return send(src, dst, out_a.at[o - 1, part], sem_a.at[k], to)

    def brick(o):
        s2 = (me + o) % 16
        src = bricks.at[:, pl.ds(pl.multiple_of(s2 * landed.shape[1], LANES), landed.shape[1])]
        rows = bricks.shape[0]
        dst = landed.at[pl.ds(pl.multiple_of(me * rows, rows), rows), :]
        if o == 0:
            return pltpu.make_async_copy(src, dst, sem_b.at[me])
        return send(src, dst, out_b.at[o - 1], sem_b.at[me], (rb, s2))

    for part in range(2):
        for o in range(4):
            reshard(o, part).start()
    for o in range(16):
        brick(o).start()

    def first_hop(k):
        return (
            send(xs.at[c, 0, k], xs.at[c, 3, k], out_x.at[0, k], sem_x.at[0, k], right),
            send(xs.at[c, 0, k], xs.at[c, 1, k], out_x.at[1, k], sem_x.at[1, k], left),
        )

    def first_share(k):
        return (send(xs.at[c, 0, k], xs.at[c, 0, k], out_s.at[0, k], sem_s.at[0, k], twin),)

    def second_hop(k):
        lo_rows, hi_rows = pl.ds(0, half), pl.ds(half, half)
        return (
            send(xs.at[c, 3, k, lo_rows], xs.at[c, 2, k, lo_rows], out_h.at[0, k], sem_h.at[0, k], right),
            send(xs.at[c, 1, k, hi_rows], xs.at[c, 2, k, hi_rows], out_h.at[1, k], sem_h.at[1, k], left),
            send(xs.at[c, 3, k], xs.at[c, 3, k], out_s.at[3, k], sem_s.at[3, k], twin),
            send(xs.at[c, 1, k], xs.at[c, 1, k], out_s.at[1, k], sem_s.at[1, k], twin),
        )

    def last_share(k):
        return (send(xs.at[c, 2, k], xs.at[c, 2, k], out_s.at[2, k], sem_s.at[2, k], twin),)

    own = ps.shape[2]
    top, bottom = pl.ds(0, own // 2), pl.ds(own // 2, own // 2)

    def slot_of(j):
        return (j - x + 2 * NX) % NX

    def hop(h, k):
        dp, dm = slot_of(z - h), slot_of(z + h)
        return (
            send(ps.at[k, dp, top], zp.at[k, h - 1], out_p.at[k, h - 1], sem_p.at[k, h - 1], up),
            send(ps.at[k, dm, bottom], zm.at[k, h - 1], out_m.at[k, h - 1], sem_m.at[k, h - 1], down),
        )

    def add_in(h, k):
        dp, dm = slot_of(z - h), slot_of(z + h)
        arrived(zp.at[k, h - 2], sem_p.at[k, h - 2])
        ps[k, dp, top] = ps[k, dp, top] + zp[k, h - 2]
        arrived(zm.at[k, h - 2], sem_m.at[k, h - 2])
        ps[k, dm, bottom] = ps[k, dm, bottom] + zm[k, h - 2]

    def y_send(b, k):
        yr = (k % 2) * 2 + b
        slot = (y - yr + 8) % 4 - 1
        rows = top if b == 0 else bottom
        to = (z * 2 + k % 2, snap_of(x, b, c))
        return yr, send(
            ps.at[k, slot_of(z), rows], ys.at[k // 2, slot], out_y.at[b, k], sem_y.at[k // 2, slot], to
        )

    def issue(copies):
        for copy in copies:
            copy.start()

    def own_operand():
        for yl in range(2):
            for part in range(2):
                k = part * 4 + c * 2 + yl
                for s in range(2):
                    w = w_ref[:, pl.ds(pl.multiple_of(y_lo * 2 * depth + s * depth, LANES), depth)]
                    block = xs[s, 0, k].T * (w * scale)
                    hi = block.astype(jnp.bfloat16)
                    rows = pl.ds((yl * 2 + part) * LANES, LANES)
                    cols = pl.ds(s * depth, depth)
                    ahi[rows, cols] = hi
                    alo[rows, cols] = (block - hi.astype(jnp.float32)).astype(jnp.bfloat16)

    def split(d, k, at):
        for s in range(2):
            block = xs[s, d, k]
            hi = block.astype(jnp.bfloat16)
            rows, cols = pl.ds(s * depth, depth), pl.ds(at, LANES)
            bhi[rows, cols] = hi
            blo[rows, cols] = (block - hi.astype(jnp.float32)).astype(jnp.bfloat16)

    def product(at, n):
        cols = pl.ds(at, n)
        dot = functools.partial(jnp.dot, preferred_element_type=jnp.float32)
        a, b = ahi[...], bhi[:, cols]
        return dot(a, b) + (dot(a, blo[:, cols]) + dot(alo[...], b))

    def step(i, carry):
        @pl.when(i >= 5)
        def _():
            k = i - 5

            @pl.when(y_hi == k % 2)
            def _():
                for slot in range(3):
                    arrived(ys.at[k // 2, slot], sem_y.at[k // 2, slot])
                mine = ps[k, slot_of(z), pl.ds(pl.multiple_of(y_lo * (own // 2), own // 2), own // 2)]
                total = mine + (ys[k // 2, 0] + (ys[k // 2, 1] + ys[k // 2, 2]))
                at = ((k // 2) % 2) * 256 + (k // 4) * LANES
                gram[pl.ds(pl.multiple_of(at, LANES), LANES), :] = total.T

        @pl.when((i >= 4) & (i < CHUNKS + 4))
        def _():
            k = i - 4
            add_in(4, k)
            for b in range(2):
                yr, copy = y_send(b, k)

                @pl.when(y != yr)
                def _():
                    copy.start()

        for h in (3, 2):
            @pl.when((i >= h) & (i < CHUNKS + h))
            def _():
                add_in(h, i - h)
                issue(hop(h, i - h))

        @pl.when(i + 2 < CHUNKS)
        def _():
            issue(first_hop(i + 2))

        @pl.when(i < CHUNKS)
        def _():
            arrived(xs.at[c, 3, i], sem_x.at[0, i])
            arrived(xs.at[c, 1, i], sem_x.at[1, i])
            issue(second_hop(i))

        @pl.when((i >= 1) & (i < CHUNKS + 1))
        def _():
            k = i - 1
            arrived(xs.at[c, 2, k, pl.ds(0, half)], sem_h.at[0, k])
            arrived(xs.at[c, 2, k, pl.ds(half, half)], sem_h.at[1, k])
            issue(last_share(k))
            for n, d in enumerate((0, 1, 3)):
                if d:
                    arrived(xs.at[1 - c, d, k], sem_s.at[d, k])
                split(d, k, n * LANES)
            out = product(0, 3 * LANES)
            for n, d in enumerate((0, 1, 3)):
                ps[k, d] = out[:, n * LANES : (n + 1) * LANES]
            arrived(xs.at[1 - c, 2, k], sem_s.at[2, k])
            split(2, k, 3 * LANES)
            ps[k, 2] = product(3 * LANES, LANES)
            issue(hop(1, k))

        return carry

    for k in range(CHUNKS):
        arrived(xs.at[c, 0, k], sem_a.at[k])
        issue(first_share(k))
        if k < 2:
            issue(first_hop(k))
    for k in range(CHUNKS):
        arrived(xs.at[1 - c, 0, k], sem_s.at[0, k])
    own_operand()
    lax.fori_loop(0, CHUNKS + LAG, step, 0)

    for s in range(16):
        rows = bricks.shape[0]
        arrived(landed.at[pl.ds(s * rows, rows), :], sem_b.at[s])

    for part in range(2):
        for o in range(1, 4):
            reshard(o, part).wait_send()
    for o in range(1, 16):
        brick(o).wait_send()

    def drain(k, carry):
        for copy in (*first_hop(k), *first_share(k), *second_hop(k), *last_share(k), *hop(1, k), *hop(2, k), *hop(3, k)):
            copy.wait_send()
        for b in range(2):
            yr, copy = y_send(b, k)

            @pl.when(y != yr)
            def _():
                copy.wait_send()

        return carry

    lax.fori_loop(0, CHUNKS, drain, 0)


def place(order, landed, tiles, held, sem_in, sem_out):
    def moves(q):
        there = pl.ds(pl.multiple_of(order[0, q] * BRICK, BRICK), BRICK)
        here = pl.ds(pl.multiple_of(q * BRICK, BRICK), BRICK)
        return (
            pltpu.make_async_copy(landed.at[there], held.at[q], sem_in.at[q]),
            pltpu.make_async_copy(held.at[q], tiles.at[here], sem_out.at[q]),
        )

    count = held.shape[0]
    for q in range(count):
        moves(q)[0].start()
    for q in range(count):
        into, out = moves(q)
        into.wait()
        out.start()
    for q in range(count):
        moves(q)[1].wait()


def per_device(snapshots, weights, next_bricks, brick_source):
    rows, width = snapshots.shape
    depth, own = rows // 4, 2 * width
    scale = 1.0 / math.sqrt(rows * lax.axis_size("rows"))
    f32, bf16, dma = jnp.float32, jnp.bfloat16, pltpu.SemaphoreType.DMA
    vmem = pltpu.VMEM
    space = lambda kind: pl.BlockSpec(memory_space=kind)
    gram, landed = pl.pallas_call(
        functools.partial(kernel, scale),
        out_shape=(
            jax.ShapeDtypeStruct((2 * width, width), f32),
            jax.ShapeDtypeStruct((rows, width), f32),
        ),
        in_specs=[space(pl.ANY), space(vmem), space(pl.ANY)],
        out_specs=(space(vmem), space(pl.ANY)),
        scratch_shapes=[
            vmem((2, 4, CHUNKS, depth, LANES), f32),
            vmem((own, 2 * depth), bf16),
            vmem((own, 2 * depth), bf16),
            vmem((2 * depth, 4 * LANES), bf16),
            vmem((2 * depth, 4 * LANES), bf16),
            vmem((CHUNKS, 4, own, LANES), f32),
            vmem((CHUNKS, 3, own // 2, LANES), f32),
            vmem((CHUNKS, 3, own // 2, LANES), f32),
            vmem((CHUNKS // 2, 3, own // 2, LANES), f32),
            dma((CHUNKS,)), dma((2, CHUNKS)), dma((2, CHUNKS)), dma((4, CHUNKS)),
            dma((CHUNKS, 3)), dma((CHUNKS, 3)), dma((CHUNKS // 2, 3)), dma((16,)),
            dma((3, 2)), dma((2, CHUNKS)), dma((2, CHUNKS)), dma((4, CHUNKS)),
            dma((CHUNKS, 3)), dma((CHUNKS, 3)), dma((2, CHUNKS)), dma((15,)),
        ],
        compiler_params=pltpu.CompilerParams(
            collective_id=0, has_side_effects=True, vmem_limit_bytes=60 * 1024 * 1024
        ),
    )(snapshots, weights.reshape(1, rows), next_bricks)
    count = rows // BRICK
    tiles = pl.pallas_call(
        place,
        out_shape=jax.ShapeDtypeStruct((rows, width), f32),
        in_specs=[space(pltpu.SMEM), space(pl.ANY)],
        out_specs=space(pl.ANY),
        scratch_shapes=[vmem((count, BRICK, width), f32), dma((count,)), dma((count,))],
    )(brick_source, landed)
    return gram, tiles


def solution(mesh):
    return jax.shard_map(
        per_device,
        mesh=mesh,
        in_specs=(P("rows", "snaps"), P("rows"), P(("rows", "snaps"), None), P("rows", None)),
        out_specs=(P("rows", "snaps"), P("rows", "snaps")),
        check_vma=False,
    )
```

```python
import functools
import math

import jax
import jax.numpy as jnp
from jax import lax
from jax.experimental import pallas as pl
from jax.experimental.pallas import tpu as pltpu
from jax.sharding import PartitionSpec as P

BRICK = 32
NX, NZ = 4, 4
CHUNKS = 8
LANES = 128
LAG = 4
MESH = pl.DeviceIdType.MESH


def kernel(
    scale, snap, w_ref, bricks, gram, landed,
    xs, ahi, alo, bhi, blo, ps, zs, ys,
    sem_a, sem_x, sem_h, sem_s, sem_z, sem_y, sem_b,
    out_a, out_x, out_h, out_s, out_z, out_y, out_b,
):
    rb, me = lax.axis_index("rows"), lax.axis_index("snaps")
    z, y_hi = rb // 2, rb % 2
    x, y_lo, c = me // 4, (me // 2) % 2, me % 2
    y = y_hi * 2 + y_lo
    quarter = y_lo * 2 + c
    depth = xs.shape[3]
    half = depth // 2

    def snap_of(xx, yl, cc):
        return xx * 4 + yl * 2 + cc

    right = (rb, snap_of((x + 1) % NX, y_lo, c))
    left = (rb, snap_of((x + 3) % NX, y_lo, c))
    twin = (rb, snap_of(x, y_lo, 1 - c))
    up = (((z + 1) % NZ) * 2 + y_hi, me)
    down = (((z + 3) % NZ) * 2 + y_hi, me)

    def send(src, dst, s_sem, r_sem, to):
        return pltpu.make_async_remote_copy(
            src_ref=src, dst_ref=dst, send_sem=s_sem, recv_sem=r_sem, device_id=to, device_id_type=MESH
        )

    def arrived(dst, sem):
        pltpu.make_async_copy(dst, dst, sem).wait()

    barrier = pltpu.get_barrier_semaphore()
    for o in range(1, 16):
        pl.semaphore_signal(barrier, inc=1, device_id=(rb, (me + o) % 16), device_id_type=MESH)
    pl.semaphore_signal(barrier, inc=1, device_id=up, device_id_type=MESH)
    pl.semaphore_signal(barrier, inc=1, device_id=down, device_id_type=MESH)
    for yl in range(2):
        far = (z * 2 + 1 - y_hi, snap_of(x, yl, c))
        pl.semaphore_signal(barrier, inc=1, device_id=far, device_id_type=MESH)
    pl.semaphore_wait(barrier, 19)

    def reshard(o, part):
        q2 = (quarter + o) % 4
        k = part * 4 + c * 2 + y_lo
        src = snap.at[pl.ds(pl.multiple_of(q2 * depth, depth), depth), pl.ds(part * LANES, LANES)]
        dst = xs.at[q2 % 2, 0, k]
        if o == 0:
            return pltpu.make_async_copy(src, dst, sem_a.at[k])
        to = (rb, snap_of(x, q2 // 2, q2 % 2))
        return send(src, dst, out_a.at[o - 1, part], sem_a.at[k], to)

    def brick(o):
        dx, dy, dc = o // 4, (o // 2) % 2, o % 2
        s2 = snap_of((x + dx) % NX, (y_lo + dy) % 2, (c + dc) % 2)
        src = bricks.at[:, pl.ds(pl.multiple_of(s2 * landed.shape[1], LANES), landed.shape[1])]
        rows = bricks.shape[0]
        dst = landed.at[pl.ds(pl.multiple_of(me * rows, rows), rows), :]
        if isinstance(o, int) and o == 0:
            return pltpu.make_async_copy(src, dst, sem_b.at[me])
        return send(src, dst, out_b.at[o - 1], sem_b.at[me], (rb, s2))

    for part in range(2):
        for o in range(4):
            reshard(o, part).start()
    for o in range(16):
        if (o // 2) % 2 == 0:
            brick(o).start()

    def first_hop(k):
        return (
            send(xs.at[c, 0, k], xs.at[c, 3, k], out_x.at[0, k], sem_x.at[0, k], right),
            send(xs.at[c, 0, k], xs.at[c, 1, k], out_x.at[1, k], sem_x.at[1, k], left),
        )

    def first_share(k):
        return (send(xs.at[c, 0, k], xs.at[c, 0, k], out_s.at[0, k], sem_s.at[0, k], twin),)

    def second_hop(k):
        lo_rows, hi_rows = pl.ds(0, half), pl.ds(half, half)
        return (
            send(xs.at[c, 3, k, lo_rows], xs.at[c, 2, k, lo_rows], out_h.at[0, k], sem_h.at[0, k], right),
            send(xs.at[c, 1, k, hi_rows], xs.at[c, 2, k, hi_rows], out_h.at[1, k], sem_h.at[1, k], left),
            send(xs.at[c, 3, k], xs.at[c, 3, k], out_s.at[3, k], sem_s.at[3, k], twin),
            send(xs.at[c, 1, k], xs.at[c, 1, k], out_s.at[1, k], sem_s.at[1, k], twin),
        )

    def last_share(k):
        return (send(xs.at[c, 2, k], xs.at[c, 2, k], out_s.at[2, k], sem_s.at[2, k], twin),)

    own = ps.shape[2]
    top, bottom = pl.ds(0, own // 2), pl.ds(own // 2, own // 2)

    def slot_of(j):
        return (j - x + 2 * NX) % NX

    def z_send(n, k, j, rows, to):
        return send(ps.at[k, slot_of(j), rows], zs.at[n, k], out_z.at[n, k], sem_z.at[n, k], to)

    def z_first(k):
        return (
            z_send(0, k, z + 2, top, down),
            z_send(1, k, z + 2, bottom, up),
            z_send(2, k, z + 1, top, up),
            z_send(3, k, z - 1, bottom, down),
        )

    def z_second(k):
        return (z_send(4, k, z - 1, top, down), z_send(5, k, z + 1, bottom, up))

    def z_add(k, j, rows, ns):
        d = slot_of(j)
        total = ps[k, d, rows]
        for n in ns:
            arrived(zs.at[n, k], sem_z.at[n, k])
            total = total + zs[n, k]
        ps[k, d, rows] = total

    def y_send(b, k):
        yr = (k % 2) * 2 + b
        slot = (y - yr + 8) % 4 - 1
        rows = top if b == 0 else bottom
        to = (z * 2 + k % 2, snap_of(x, b, c))
        return yr, send(
            ps.at[k, slot_of(z), rows], ys.at[k // 2, slot], out_y.at[b, k], sem_y.at[k // 2, slot], to
        )

    def issue(copies):
        for copy in copies:
            copy.start()

    def own_operand():
        for yl in range(2):
            for part in range(2):
                k = part * 4 + c * 2 + yl
                for s in range(2):
                    w = w_ref[:, pl.ds(pl.multiple_of(y_lo * 2 * depth + s * depth, LANES), depth)]
                    block = xs[s, 0, k].T * (w * scale)
                    hi = block.astype(jnp.bfloat16)
                    rows = pl.ds((yl * 2 + part) * LANES, LANES)
                    cols = pl.ds(s * depth, depth)
                    ahi[rows, cols] = hi
                    alo[rows, cols] = (block - hi.astype(jnp.float32)).astype(jnp.bfloat16)

    def split(d, k, at):
        for s in range(2):
            block = xs[s, d, k]
            hi = block.astype(jnp.bfloat16)
            rows, cols = pl.ds(s * depth, depth), pl.ds(at, LANES)
            bhi[rows, cols] = hi
            blo[rows, cols] = (block - hi.astype(jnp.float32)).astype(jnp.bfloat16)

    def product(at, n):
        cols = pl.ds(at, n)
        dot = functools.partial(jnp.dot, preferred_element_type=jnp.float32)
        a, b = ahi[...], bhi[:, cols]
        return dot(a, b) + (dot(a, blo[:, cols]) + dot(alo[...], b))

    def step(i, carry):
        @pl.when(i < CHUNKS)
        def _():
            arrived(xs.at[c, 3, i], sem_x.at[0, i])
            arrived(xs.at[c, 1, i], sem_x.at[1, i])
            issue(second_hop(i))
            brick((i // 2) * 4 + 2 + i % 2).start()

        @pl.when(i + 4 < CHUNKS)
        def _():
            issue(first_hop(i + 4))

        @pl.when((i >= 1) & (i < CHUNKS + 1))
        def _():
            arrived(xs.at[c, 2, i - 1, pl.ds(0, half)], sem_h.at[0, i - 1])
            arrived(xs.at[c, 2, i - 1, pl.ds(half, half)], sem_h.at[1, i - 1])
            issue(last_share(i - 1))

        @pl.when(i < CHUNKS)
        def _():
            arrived(xs.at[1 - c, 1, i], sem_s.at[1, i])
            arrived(xs.at[1 - c, 3, i], sem_s.at[3, i])
            for n, d in enumerate((0, 1, 3)):
                split(d, i, n * LANES)
            out = product(0, 3 * LANES)
            for n, d in enumerate((0, 1, 3)):
                ps[i, d] = out[:, n * LANES : (n + 1) * LANES]

        @pl.when((i >= 1) & (i < CHUNKS + 1))
        def _():
            k = i - 1
            arrived(xs.at[1 - c, 2, k], sem_s.at[2, k])
            split(2, k, 3 * LANES)
            ps[k, 2] = product(3 * LANES, LANES)
            issue(z_first(k))

        @pl.when((i >= 2) & (i < CHUNKS + 2))
        def _():
            k = i - 2
            z_add(k, z - 1, top, (0,))
            z_add(k, z + 1, bottom, (1,))
            issue(z_second(k))

        @pl.when((i >= 3) & (i < CHUNKS + 3))
        def _():
            k = i - 3
            z_add(k, z, top, (2, 4))
            z_add(k, z, bottom, (3, 5))
            for b in range(2):
                yr, copy = y_send(b, k)

                @pl.when(y != yr)
                def _():
                    copy.start()

        @pl.when(i >= 4)
        def _():
            k = i - 4

            @pl.when(y_hi == k % 2)
            def _():
                for slot in range(3):
                    arrived(ys.at[k // 2, slot], sem_y.at[k // 2, slot])
                mine = ps[k, slot_of(z), pl.ds(pl.multiple_of(y_lo * (own // 2), own // 2), own // 2)]
                total = mine + (ys[k // 2, 0] + (ys[k // 2, 1] + ys[k // 2, 2]))
                at = ((k // 2) % 2) * 256 + (k // 4) * LANES
                gram[pl.ds(pl.multiple_of(at, LANES), LANES), :] = total.T

        return carry

    for part in range(2):
        for far in range(2):
            for cc in range(2):
                k = part * 4 + cc * 2 + (y_lo + far) % 2
                arrived(xs.at[c, 0, k], sem_a.at[k])
                issue(first_share(k))
                if part == 0:
                    issue(first_hop(k))
    for k in range(CHUNKS):
        arrived(xs.at[1 - c, 0, k], sem_s.at[0, k])
    own_operand()
    lax.fori_loop(0, CHUNKS + LAG, step, 0)

    for s in range(16):
        rows = bricks.shape[0]
        arrived(landed.at[pl.ds(s * rows, rows), :], sem_b.at[s])

    for part in range(2):
        for o in range(1, 4):
            reshard(o, part).wait_send()
    for o in range(1, 16):
        brick(o).wait_send()

    def drain(k, carry):
        for copy in (*first_hop(k), *first_share(k), *second_hop(k), *last_share(k), *z_first(k), *z_second(k)):
            copy.wait_send()
        for b in range(2):
            yr, copy = y_send(b, k)

            @pl.when(y != yr)
            def _():
                copy.wait_send()

        return carry

    lax.fori_loop(0, CHUNKS, drain, 0)


def place(order, landed, tiles, held, sem_in, sem_out):
    def moves(q):
        there = pl.ds(pl.multiple_of(order[0, q] * BRICK, BRICK), BRICK)
        here = pl.ds(pl.multiple_of(q * BRICK, BRICK), BRICK)
        return (
            pltpu.make_async_copy(landed.at[there], held.at[q], sem_in.at[q]),
            pltpu.make_async_copy(held.at[q], tiles.at[here], sem_out.at[q]),
        )

    count = held.shape[0]
    for q in range(count):
        moves(q)[0].start()
    for q in range(count):
        into, out = moves(q)
        into.wait()
        out.start()
    for q in range(count):
        moves(q)[1].wait()


def per_device(snapshots, weights, next_bricks, brick_source):
    rows, width = snapshots.shape
    depth, own = rows // 4, 2 * width
    scale = 1.0 / math.sqrt(rows * lax.axis_size("rows"))
    f32, bf16, dma = jnp.float32, jnp.bfloat16, pltpu.SemaphoreType.DMA
    vmem = pltpu.VMEM
    space = lambda kind: pl.BlockSpec(memory_space=kind)
    gram, landed = pl.pallas_call(
        functools.partial(kernel, scale),
        out_shape=(
            jax.ShapeDtypeStruct((2 * width, width), f32),
            jax.ShapeDtypeStruct((rows, width), f32),
        ),
        in_specs=[space(pl.ANY), space(vmem), space(pl.ANY)],
        out_specs=(space(vmem), space(pl.ANY)),
        scratch_shapes=[
            vmem((2, 4, CHUNKS, depth, LANES), f32),
            vmem((own, 2 * depth), bf16),
            vmem((own, 2 * depth), bf16),
            vmem((2 * depth, 4 * LANES), bf16),
            vmem((2 * depth, 4 * LANES), bf16),
            vmem((CHUNKS, 4, own, LANES), f32),
            vmem((6, CHUNKS, own // 2, LANES), f32),
            vmem((CHUNKS // 2, 3, own // 2, LANES), f32),
            dma((CHUNKS,)), dma((2, CHUNKS)), dma((2, CHUNKS)), dma((4, CHUNKS)),
            dma((6, CHUNKS)), dma((CHUNKS // 2, 3)), dma((16,)),
            dma((3, 2)), dma((2, CHUNKS)), dma((2, CHUNKS)), dma((4, CHUNKS)),
            dma((6, CHUNKS)), dma((2, CHUNKS)), dma((15,)),
        ],
        compiler_params=pltpu.CompilerParams(
            collective_id=0, has_side_effects=True, vmem_limit_bytes=60 * 1024 * 1024
        ),
    )(snapshots, weights.reshape(1, rows), next_bricks)
    count = rows // BRICK
    tiles = pl.pallas_call(
        place,
        out_shape=jax.ShapeDtypeStruct((rows, width), f32),
        in_specs=[space(pltpu.SMEM), space(pl.ANY)],
        out_specs=space(pl.ANY),
        scratch_shapes=[vmem((count, BRICK, width), f32), dma((count,)), dma((count,))],
    )(brick_source, landed)
    return gram, tiles


def solution(mesh):
    return jax.shard_map(
        per_device,
        mesh=mesh,
        in_specs=(P("rows", "snaps"), P("rows"), P(("rows", "snaps"), None), P("rows", None)),
        out_specs=(P("rows", "snaps"), P("rows", "snaps")),
        check_vma=False,
    )
```

```python
import functools
import math

import jax
import jax.numpy as jnp
from jax import lax
from jax.experimental import pallas as pl
from jax.experimental.pallas import tpu as pltpu
from jax.sharding import PartitionSpec as P

BRICK = 32
NX, NZ = 4, 4
CHUNKS = 8
LANES = 128
LAG = 3
MESH = pl.DeviceIdType.MESH


def kernel(
    scale, snap, w_ref, bricks, order, gram, tiles,
    xs, ahi, alo, bhi, blo, ps, zs, ys, landed, placed,
    sem_a, sem_x, sem_h, sem_s, sem_z, sem_y, sem_b,
    out_a, out_x, out_h, out_s, out_z, out_y, out_b, out_t,
):
    rb, me = lax.axis_index("rows"), lax.axis_index("snaps")
    z, y_hi = rb // 2, rb % 2
    x, y_lo, c = me // 4, (me // 2) % 2, me % 2
    y = y_hi * 2 + y_lo
    depth = xs.shape[3]
    half = depth // 2

    def snap_of(xx, yl, cc):
        return xx * 4 + yl * 2 + cc

    right = (rb, snap_of((x + 1) % NX, y_lo, c))
    left = (rb, snap_of((x + 3) % NX, y_lo, c))
    twin = (rb, snap_of(x, y_lo, 1 - c))
    up = (((z + 1) % NZ) * 2 + y_hi, me)
    down = (((z + 3) % NZ) * 2 + y_hi, me)

    def send(src, dst, s_sem, r_sem, to):
        return pltpu.make_async_remote_copy(
            src_ref=src, dst_ref=dst, send_sem=s_sem, recv_sem=r_sem, device_id=to, device_id_type=MESH
        )

    def arrived(dst, sem):
        pltpu.make_async_copy(dst, dst, sem).wait()

    barrier = pltpu.get_barrier_semaphore()
    for o in range(1, 16):
        pl.semaphore_signal(barrier, inc=1, device_id=(rb, (me + o) % 16), device_id_type=MESH)
    pl.semaphore_signal(barrier, inc=1, device_id=up, device_id_type=MESH)
    pl.semaphore_signal(barrier, inc=1, device_id=down, device_id_type=MESH)
    for yl in range(2):
        far = (z * 2 + 1 - y_hi, snap_of(x, yl, c))
        pl.semaphore_signal(barrier, inc=1, device_id=far, device_id_type=MESH)
    pl.semaphore_wait(barrier, 19)

    def reshard(o, part):
        y2, c2 = (y_lo + o // 2) % 2, (c + o % 2) % 2
        q2 = y2 * 2 + c2
        k = (o // 2) * 4 + part * 2 + c
        src = snap.at[pl.ds(pl.multiple_of(q2 * depth, depth), depth), pl.ds(part * LANES, LANES)]
        dst = xs.at[c2, 0, k]
        if o == 0:
            return pltpu.make_async_copy(src, dst, sem_a.at[k])
        to = (rb, snap_of(x, y2, c2))
        return send(src, dst, out_a.at[o - 1, part], sem_a.at[k], to)

    def brick(o):
        dx, dy, dc = o // 4, (o // 2) % 2, o % 2
        s2 = snap_of((x + dx) % NX, (y_lo + dy) % 2, (c + dc) % 2)
        width = landed.shape[2]
        src = bricks.at[:, :, pl.ds(pl.multiple_of(s2 * width, LANES), width)]
        count = bricks.shape[0]
        dst = landed.at[pl.ds(me * count, count)]
        if isinstance(o, int) and o == 0:
            return pltpu.make_async_copy(src, dst, sem_b.at[me])
        return send(src, dst, out_b.at[o - 1], sem_b.at[me], (rb, s2))

    for part in range(2):
        for o in (0, 1, 2, 3):
            reshard(o, part).start()
    brick(0).start()
    brick(1).start()

    def first_hop(k):
        return (
            send(xs.at[c, 0, k], xs.at[c, 3, k], out_x.at[0, k], sem_x.at[0, k], right),
            send(xs.at[c, 0, k], xs.at[c, 1, k], out_x.at[1, k], sem_x.at[1, k], left),
        )

    def first_share(k):
        return (send(xs.at[c, 0, k], xs.at[c, 0, k], out_s.at[0, k], sem_s.at[0, k], twin),)

    def second_hop(k):
        lo_rows, hi_rows = pl.ds(0, half), pl.ds(half, half)
        return (
            send(xs.at[c, 3, k, lo_rows], xs.at[c, 2, k, lo_rows], out_h.at[0, k], sem_h.at[0, k], right),
            send(xs.at[c, 1, k, hi_rows], xs.at[c, 2, k, hi_rows], out_h.at[1, k], sem_h.at[1, k], left),
            send(xs.at[c, 3, k], xs.at[c, 3, k], out_s.at[3, k], sem_s.at[3, k], twin),
            send(xs.at[c, 1, k], xs.at[c, 1, k], out_s.at[1, k], sem_s.at[1, k], twin),
        )

    def last_share(k):
        return (send(xs.at[c, 2, k], xs.at[c, 2, k], out_s.at[2, k], sem_s.at[2, k], twin),)

    own = ps.shape[2]
    top, bottom = pl.ds(0, own // 2), pl.ds(own // 2, own // 2)

    def slot_of(j):
        return (j - x + 2 * NX) % NX

    def z_send(n, k, j, rows, to):
        return send(ps.at[k, slot_of(j), rows], zs.at[n, k], out_z.at[n, k], sem_z.at[n, k], to)

    def z_first(k):
        return (
            z_send(0, k, z + 2, top, down),
            z_send(1, k, z + 2, bottom, up),
            z_send(2, k, z + 1, top, up),
            z_send(3, k, z - 1, bottom, down),
        )

    def z_second(k):
        return (z_send(4, k, z - 1, top, down), z_send(5, k, z + 1, bottom, up))

    def z_add(k, j, rows, ns):
        d = slot_of(j)
        total = ps[k, d, rows]
        for n in ns:
            arrived(zs.at[n, k], sem_z.at[n, k])
            total = total + zs[n, k]
        ps[k, d, rows] = total

    def y_send(b, k):
        h, m = (y_lo + k // 4) % 2, k % 4
        yr = h * 2 + b
        slot = (y - yr + 8) % 4 - 1
        rows = top if b == 0 else bottom
        to = (z * 2 + h, snap_of(x, b, c))
        return yr, send(ps.at[k, slot_of(z), rows], ys.at[m, slot], out_y.at[b, k], sem_y.at[m, slot], to)

    def issue(copies):
        for copy in copies:
            copy.start()

    def own_operand():
        for far in range(2):
            for part in range(2):
                k = far * 4 + part * 2 + c
                at = ((y_lo + far) % 2) * 2 * LANES + part * LANES
                rows = pl.ds(pl.multiple_of(at, LANES), LANES)
                for s in range(2):
                    w = w_ref[:, pl.ds(pl.multiple_of(y_lo * 2 * depth + s * depth, LANES), depth)]
                    block = xs[s, 0, k].T * (w * scale)
                    hi = block.astype(jnp.bfloat16)
                    cols = pl.ds(s * depth, depth)
                    ahi[rows, cols] = hi
                    alo[rows, cols] = (block - hi.astype(jnp.float32)).astype(jnp.bfloat16)

    def split(d, k, at):
        for s in range(2):
            block = xs[s, d, k]
            hi = block.astype(jnp.bfloat16)
            rows, cols = pl.ds(s * depth, depth), pl.ds(at, LANES)
            bhi[rows, cols] = hi
            blo[rows, cols] = (block - hi.astype(jnp.float32)).astype(jnp.bfloat16)

    def product():
        dot = functools.partial(jnp.dot, preferred_element_type=jnp.float32)
        a, b = ahi[...], bhi[...]
        return dot(a, b) + (dot(a, blo[...]) + dot(alo[...], b))

    def pass_on(k):
        arrived(xs.at[c, 3, k], sem_x.at[0, k])
        arrived(xs.at[c, 1, k], sem_x.at[1, k])
        issue(second_hop(k))

    def pass_last(k):
        arrived(xs.at[c, 2, k, pl.ds(0, half)], sem_h.at[0, k])
        arrived(xs.at[c, 2, k, pl.ds(half, half)], sem_h.at[1, k])
        issue(last_share(k))

    def step(i, carry):
        @pl.when(i < CHUNKS)
        def _():
            for d in (1, 2, 3):
                arrived(xs.at[1 - c, d, i], sem_s.at[d, i])
            for d in range(4):
                split(d, i, d * LANES)
            out = product()
            for d in range(4):
                ps[i, d] = out[:, d * LANES : (d + 1) * LANES]
            issue(z_first(i))

        @pl.when(i + 3 < CHUNKS)
        def _():
            pass_on(i + 3)

        @pl.when(i + 5 < CHUNKS)
        def _():
            issue(first_hop(i + 5))

        @pl.when(i + 3 == CHUNKS - 1)
        def _():
            for n in range(4, 16):
                brick(n).start()

        @pl.when(i + 2 < CHUNKS)
        def _():
            pass_last(i + 2)

        @pl.when((i >= 1) & (i < CHUNKS + 1))
        def _():
            k = i - 1
            z_add(k, z - 1, top, (0,))
            z_add(k, z + 1, bottom, (1,))
            issue(z_second(k))

        @pl.when((i >= 2) & (i < CHUNKS + 2))
        def _():
            k = i - 2
            z_add(k, z, top, (2, 4))
            z_add(k, z, bottom, (3, 5))
            for b in range(2):
                yr, copy = y_send(b, k)

                @pl.when(y != yr)
                def _():
                    copy.start()

        @pl.when(i >= 4 + LAG)
        def _():
            m = i - 4 - LAG
            k = ((y_hi + y_lo) % 2) * 4 + m
            for slot in range(3):
                arrived(ys.at[m, slot], sem_y.at[m, slot])
            mine = ps[k, slot_of(z), pl.ds(pl.multiple_of(y_lo * (own // 2), own // 2), own // 2)]
            total = mine + (ys[m, 0] + (ys[m, 1] + ys[m, 2]))
            at = (m % 2) * 2 * LANES + (m // 2) * LANES
            gram[pl.ds(pl.multiple_of(at, LANES), LANES), :] = total.T

        return carry

    def ready(k):
        arrived(xs.at[c, 0, k], sem_a.at[k])
        issue(first_share(k))

    for k in range(4):
        ready(k)
        if k < 2:
            issue(first_hop(k))
    pass_on(0)
    issue(first_hop(2))
    pass_on(1)
    issue(first_hop(3))
    pass_last(0)
    ready(4)
    ready(5)
    pass_on(2)
    issue(first_hop(4))
    pass_last(1)
    ready(6)
    ready(7)
    brick(2).start()
    brick(3).start()
    for k in range(CHUNKS):
        arrived(xs.at[1 - c, 0, k], sem_s.at[0, k])
    own_operand()
    lax.fori_loop(0, CHUNKS + 1, step, 0)
    count = bricks.shape[0]
    for s in range(16):
        arrived(landed.at[pl.ds(s * count, count)], sem_b.at[s])

    def place(q, carry):
        placed[q] = landed[order[0, q]]
        return carry

    lax.fori_loop(0, placed.shape[0], place, 0)
    written = pltpu.make_async_copy(placed, tiles, out_t)
    written.start()
    lax.fori_loop(CHUNKS + 1, CHUNKS + LAG, step, 0)
    written.wait()

    for part in range(2):
        for o in range(1, 4):
            reshard(o, part).wait_send()
    for o in range(1, 16):
        brick(o).wait_send()

    def drain(k, carry):
        for copy in (*first_hop(k), *first_share(k), *second_hop(k), *last_share(k), *z_first(k), *z_second(k)):
            copy.wait_send()
        for b in range(2):
            yr, copy = y_send(b, k)

            @pl.when(y != yr)
            def _():
                copy.wait_send()

        return carry

    lax.fori_loop(0, CHUNKS, drain, 0)


def per_device(snapshots, weights, next_bricks, brick_source):
    rows, width = snapshots.shape
    depth, own = rows // 4, 2 * width
    scale = 1.0 / math.sqrt(rows * lax.axis_size("rows"))
    f32, bf16, dma = jnp.float32, jnp.bfloat16, pltpu.SemaphoreType.DMA
    vmem = pltpu.VMEM
    space = lambda kind: pl.BlockSpec(memory_space=kind)
    count = rows // BRICK
    gram, tiles = pl.pallas_call(
        functools.partial(kernel, scale),
        out_shape=(
            jax.ShapeDtypeStruct((2 * width, width), f32),
            jax.ShapeDtypeStruct((count, BRICK, width), f32),
        ),
        in_specs=[space(pl.ANY), space(vmem), space(pl.ANY), space(pltpu.SMEM)],
        out_specs=(space(vmem), space(pl.ANY)),
        scratch_shapes=[
            vmem((2, 4, CHUNKS, depth, LANES), f32),
            vmem((own, 2 * depth), bf16),
            vmem((own, 2 * depth), bf16),
            vmem((2 * depth, 4 * LANES), bf16),
            vmem((2 * depth, 4 * LANES), bf16),
            vmem((CHUNKS, 4, own, LANES), f32),
            vmem((6, CHUNKS, own // 2, LANES), f32),
            vmem((CHUNKS // 2, 3, own // 2, LANES), f32),
            vmem((count, BRICK, width), f32),
            vmem((count, BRICK, width), f32),
            dma((CHUNKS,)), dma((2, CHUNKS)), dma((2, CHUNKS)), dma((4, CHUNKS)),
            dma((6, CHUNKS)), dma((CHUNKS // 2, 3)), dma((16,)),
            dma((3, 2)), dma((2, CHUNKS)), dma((2, CHUNKS)), dma((4, CHUNKS)),
            dma((6, CHUNKS)), dma((2, CHUNKS)), dma((15,)), dma,
        ],
        compiler_params=pltpu.CompilerParams(
            collective_id=0, has_side_effects=True, vmem_limit_bytes=60 * 1024 * 1024
        ),
    )(snapshots, weights.reshape(1, rows), next_bricks.reshape(-1, BRICK, next_bricks.shape[1]), brick_source)
    return gram, tiles.reshape(rows, width)


def solution(mesh):
    return jax.shard_map(
        per_device,
        mesh=mesh,
        in_specs=(P("rows", "snaps"), P("rows"), P(("rows", "snaps"), None), P("rows", None)),
        out_specs=(P("rows", "snaps"), P("rows", "snaps")),
        check_vma=False,
    )
```

```python
import functools
import math

import jax
import jax.numpy as jnp
from jax import lax
from jax.experimental import pallas as pl
from jax.experimental.pallas import tpu as pltpu
from jax.sharding import PartitionSpec as P

BRICK = 32
NX, NZ = 4, 4
CHUNKS = 8
LANES = 128
LAG = 3
EARLY = 2
MESH = pl.DeviceIdType.MESH


def kernel(
    scale, snap, w_ref, bricks, order, gram, tiles,
    xs, ahi, alo, bhi, blo, ps, zs, ys, landed, relay, across,
    sem_a, sem_x, sem_h, sem_s, sem_z, sem_y, sem_b, sem_r, sem_o,
    out_a, out_x, out_h, out_s, out_z, out_y, out_b, out_r, out_o, out_n,
):
    rb, me = lax.axis_index("rows"), lax.axis_index("snaps")
    z, y_hi = rb // 2, rb % 2
    x, y_lo, c = me // 4, (me // 2) % 2, me % 2
    y = y_hi * 2 + y_lo
    depth = xs.shape[3]
    half = depth // 2

    def snap_of(xx, yl, cc):
        return xx * 4 + yl * 2 + cc

    right = (rb, snap_of((x + 1) % NX, y_lo, c))
    left = (rb, snap_of((x + 3) % NX, y_lo, c))
    twin = (rb, snap_of(x, y_lo, 1 - c))
    up = (((z + 1) % NZ) * 2 + y_hi, me)
    down = (((z + 3) % NZ) * 2 + y_hi, me)

    def send(src, dst, s_sem, r_sem, to):
        return pltpu.make_async_remote_copy(
            src_ref=src, dst_ref=dst, send_sem=s_sem, recv_sem=r_sem, device_id=to, device_id_type=MESH
        )

    def arrived(dst, sem):
        pltpu.make_async_copy(dst, dst, sem).wait()

    barrier = pltpu.get_barrier_semaphore()
    for o in range(1, 16):
        pl.semaphore_signal(barrier, inc=1, device_id=(rb, (me + o) % 16), device_id_type=MESH)
    pl.semaphore_signal(barrier, inc=1, device_id=up, device_id_type=MESH)
    pl.semaphore_signal(barrier, inc=1, device_id=down, device_id_type=MESH)
    for yl in range(2):
        far = (z * 2 + 1 - y_hi, snap_of(x, yl, c))
        pl.semaphore_signal(barrier, inc=1, device_id=far, device_id_type=MESH)
    pl.semaphore_wait(barrier, 19)

    def reshard(o, part):
        y2, c2 = (y_lo + o // 2) % 2, (c + o % 2) % 2
        q2 = y2 * 2 + c2
        k = (o // 2) * 4 + part * 2 + c
        src = snap.at[pl.ds(pl.multiple_of(q2 * depth, depth), depth), pl.ds(part * LANES, LANES)]
        dst = xs.at[c2, 0, k]
        if o == 0:
            return pltpu.make_async_copy(src, dst, sem_a.at[k])
        to = (rb, snap_of(x, y2, c2))
        return send(src, dst, out_a.at[o - 1, part], sem_a.at[k], to)

    def brick(o):
        s2 = snap_of(x, (y_lo + o // 2) % 2, (c + o % 2) % 2)
        width = landed.shape[2]
        src = bricks.at[:, :, pl.ds(pl.multiple_of(s2 * width, LANES), width)]
        count = bricks.shape[0]
        dst = landed.at[pl.ds(me * count, count)]
        if o == 0:
            return pltpu.make_async_copy(src, dst, sem_b.at[me])
        return send(src, dst, out_b.at[o - 1], sem_b.at[me], (rb, s2))

    def brick_cols(dx, dy, dc):
        width = landed.shape[2]
        s2 = snap_of((x + dx) % NX, (y_lo + dy) % 2, (c + dc) % 2)
        return bricks.at[:, :, pl.ds(pl.multiple_of(s2 * width, LANES), width)]

    def rows_from(source):
        return landed.at[pl.ds(source * bricks.shape[0], bricks.shape[0])]

    def brick_over(dx, dc):
        to = (rb, snap_of(x, 1 - y_lo, c))
        dst = across.at[dx - 1, dc]
        return send(brick_cols(dx, 1, dc), dst, out_o.at[dx - 1, dc], sem_o.at[dx - 1, dc], to)

    def held_bricks(dx, dy, dc):
        return across.at[dx - 1, dc] if dy else brick_cols(dx, 0, dc)

    def brick_near(dx, dy, dc):
        source = snap_of(x, (y_lo + dy) % 2, c)
        to = (rb, snap_of((x + dx) % NX, y_lo, (c + dc) % 2))
        sem = out_n.at[dx // 2, dy, dc]
        return send(held_bricks(dx, dy, dc), rows_from(source), sem, sem_b.at[source], to)

    def brick_far(g, dy):
        ahead, behind = (x + 1 + 2 * g) % NX, (x + 3 - 2 * g) % NX
        source = snap_of(behind, (y_lo + dy) % 2, c)
        to = (rb, snap_of(ahead, y_lo, (c + g) % 2))
        hop = send(
            held_bricks(2, dy, g), relay.at[g, dy], out_r.at[0, g, dy], sem_r.at[g, dy], left if g else right
        )
        return hop, send(relay.at[g, dy], rows_from(source), out_r.at[1, g, dy], sem_b.at[source], to)

    near = [(dx, dy, dc) for dx in (1, 3) for dy in range(2) for dc in range(2)]
    over = [(dx, dc) for dx in (1, 2, 3) for dc in range(2)]

    for part in range(2):
        for o in (0, 1, 2, 3):
            reshard(o, part).start()
    brick(0).start()
    brick(1).start()

    def first_hop(k):
        return (
            send(xs.at[c, 0, k], xs.at[c, 3, k], out_x.at[0, k], sem_x.at[0, k], right),
            send(xs.at[c, 0, k], xs.at[c, 1, k], out_x.at[1, k], sem_x.at[1, k], left),
        )

    def first_share(k):
        return (send(xs.at[c, 0, k], xs.at[c, 0, k], out_s.at[0, k], sem_s.at[0, k], twin),)

    def second_hop(k):
        lo_rows, hi_rows = pl.ds(0, half), pl.ds(half, half)
        return (
            send(xs.at[c, 3, k, lo_rows], xs.at[c, 2, k, lo_rows], out_h.at[0, k], sem_h.at[0, k], right),
            send(xs.at[c, 1, k, hi_rows], xs.at[c, 2, k, hi_rows], out_h.at[1, k], sem_h.at[1, k], left),
            send(xs.at[c, 3, k], xs.at[c, 3, k], out_s.at[3, k], sem_s.at[3, k], twin),
            send(xs.at[c, 1, k], xs.at[c, 1, k], out_s.at[1, k], sem_s.at[1, k], twin),
        )

    def last_share(k):
        return (send(xs.at[c, 2, k], xs.at[c, 2, k], out_s.at[2, k], sem_s.at[2, k], twin),)

    own = ps.shape[2]
    top, bottom = pl.ds(0, own // 2), pl.ds(own // 2, own // 2)

    def slot_of(j):
        return (j - x + 2 * NX) % NX

    def z_send(n, k, j, rows, to):
        return send(ps.at[k, slot_of(j), rows], zs.at[n, k], out_z.at[n, k], sem_z.at[n, k], to)

    def z_first(k, b):
        if b == 0:
            return (z_send(0, k, z + 2, top, down), z_send(2, k, z + 1, top, up))
        return (z_send(1, k, z + 2, bottom, up), z_send(3, k, z - 1, bottom, down))

    def z_second(k):
        return (z_send(4, k, z - 1, top, down), z_send(5, k, z + 1, bottom, up))

    def z_add(k, j, rows, ns):
        d = slot_of(j)
        total = ps[k, d, rows]
        for n in ns:
            arrived(zs.at[n, k], sem_z.at[n, k])
            total = total + zs[n, k]
        ps[k, d, rows] = total

    def y_send(b, k):
        h, m = (y_lo + k // 4) % 2, k % 4
        yr = h * 2 + b
        slot = (y - yr + 8) % 4 - 1
        rows = top if b == 0 else bottom
        to = (z * 2 + h, snap_of(x, b, c))
        return yr, send(ps.at[k, slot_of(z), rows], ys.at[m, slot], out_y.at[b, k], sem_y.at[m, slot], to)

    def issue(copies):
        for copy in copies:
            copy.start()

    def own_operand(far):
        for part in range(2):
            k = far * 4 + part * 2 + c
            at = ((y_lo + far) % 2) * 2 * LANES + part * LANES
            rows = pl.ds(pl.multiple_of(at, LANES), LANES)
            for s in range(2):
                w = w_ref[:, pl.ds(pl.multiple_of(y_lo * 2 * depth + s * depth, LANES), depth)]
                block = xs[s, 0, k].T * (w * scale)
                hi = block.astype(jnp.bfloat16)
                cols = pl.ds(s * depth, depth)
                ahi[rows, cols] = hi
                alo[rows, cols] = (block - hi.astype(jnp.float32)).astype(jnp.bfloat16)

    def split(d, k, at):
        for s in range(2):
            block = xs[s, d, k]
            hi = block.astype(jnp.bfloat16)
            rows, cols = pl.ds(s * depth, depth), pl.ds(at, LANES)
            bhi[rows, cols] = hi
            blo[rows, cols] = (block - hi.astype(jnp.float32)).astype(jnp.bfloat16)

    def product(k, far):
        dot = functools.partial(jnp.dot, preferred_element_type=jnp.float32)
        size = own // 2
        rows = pl.ds(pl.multiple_of(((y_lo + far) % 2) * size, size), size)
        a, b = ahi[rows, :], bhi[...]
        out = dot(a, b) + (dot(a, blo[...]) + dot(alo[rows, :], b))
        for d in range(4):
            ps[k, d, rows] = out[:, d * LANES : (d + 1) * LANES]

    def gathered(k):
        for d in (1, 2, 3):
            arrived(xs.at[1 - c, d, k], sem_s.at[d, k])
        for d in range(4):
            split(d, k, d * LANES)

    def early(k):
        gathered(k)
        product(k, 0)
        for b in range(2):

            @pl.when(y_lo == b)
            def _():
                issue(z_first(k, b))

    def pass_on(k):
        arrived(xs.at[c, 3, k], sem_x.at[0, k])
        arrived(xs.at[c, 1, k], sem_x.at[1, k])
        issue(second_hop(k))

    def pass_last(k):
        arrived(xs.at[c, 2, k, pl.ds(0, half)], sem_h.at[0, k])
        arrived(xs.at[c, 2, k, pl.ds(half, half)], sem_h.at[1, k])
        issue(last_share(k))

    def step(i, carry):
        @pl.when((i >= EARLY) & (i < CHUNKS))
        def _():
            gathered(i)
            product(i, 0)

        @pl.when(i < EARLY)
        def _():
            for d in range(4):
                split(d, i, d * LANES)

        @pl.when(i < CHUNKS)
        def _():
            product(i, 1)
            for b in range(2):

                @pl.when((i >= EARLY) | (y_lo != b))
                def _():
                    issue(z_first(i, b))

        @pl.when((i >= 1) & (i + 2 < CHUNKS))
        def _():
            pass_on(i + 2)

        @pl.when((i >= 1) & (i + 4 < CHUNKS))
        def _():
            issue(first_hop(i + 4))

        @pl.when(i + 2 == CHUNKS - 1)
        def _():
            for dx, dc in over:
                arrived(across.at[dx - 1, dc], sem_o.at[dx - 1, dc])
            for n in range(4):
                brick_far(n % 2, n // 2)[0].start()
            for at in near:
                brick_near(*at).start()

        @pl.when((i >= 1) & (i + 1 < CHUNKS))
        def _():
            pass_last(i + 1)

        @pl.when((i >= 1) & (i < CHUNKS + 1))
        def _():
            k = i - 1
            z_add(k, z - 1, top, (0,))
            z_add(k, z + 1, bottom, (1,))
            issue(z_second(k))

        @pl.when((i >= 2) & (i < CHUNKS + 2))
        def _():
            k = i - 2
            z_add(k, z, top, (2, 4))
            z_add(k, z, bottom, (3, 5))
            for b in range(2):
                yr, copy = y_send(b, k)

                @pl.when(y != yr)
                def _():
                    copy.start()

        @pl.when(i == CHUNKS - 2)
        def _():
            for n in range(4):
                g, dy = n // 2, n % 2
                arrived(relay.at[g, dy], sem_r.at[g, dy])
                brick_far(g, dy)[1].start()

        @pl.when(i >= 4 + LAG)
        def _():
            m = i - 4 - LAG
            k = ((y_hi + y_lo) % 2) * 4 + m
            for slot in range(3):
                arrived(ys.at[m, slot], sem_y.at[m, slot])
            mine = ps[k, slot_of(z), pl.ds(pl.multiple_of(y_lo * (own // 2), own // 2), own // 2)]
            total = mine + (ys[m, 0] + (ys[m, 1] + ys[m, 2]))
            at = (m % 2) * 2 * LANES + (m // 2) * LANES
            gram[pl.ds(pl.multiple_of(at, LANES), LANES), :] = total.T

        return carry

    def ready(k):
        arrived(xs.at[c, 0, k], sem_a.at[k])
        issue(first_share(k))

    for k in range(4):
        ready(k)
        if k < 2:
            issue(first_hop(k))
    for k in range(4):
        arrived(xs.at[1 - c, 0, k], sem_s.at[0, k])
    own_operand(0)
    pass_on(0)
    issue(first_hop(2))
    pass_on(1)
    issue(first_hop(3))
    pass_last(0)
    ready(4)
    ready(5)
    early(0)
    pass_on(2)
    issue(first_hop(4))
    pass_last(1)
    ready(6)
    ready(7)
    early(1)
    brick(2).start()
    brick(3).start()
    for at in over:
        brick_over(*at).start()
    for k in range(4, CHUNKS):
        arrived(xs.at[1 - c, 0, k], sem_s.at[0, k])
    own_operand(1)
    lax.fori_loop(0, CHUNKS + 1, step, 0)
    count = bricks.shape[0]
    for s in range(16):
        arrived(landed.at[pl.ds(s * count, count)], sem_b.at[s])

    def place(q, carry):
        tiles[q] = landed[order[0, q]]
        return carry

    lax.fori_loop(0, tiles.shape[0], place, 0)
    lax.fori_loop(CHUNKS + 1, CHUNKS + LAG, step, 0)

    for part in range(2):
        for o in range(1, 4):
            reshard(o, part).wait_send()
    for o in (1, 2, 3):
        brick(o).wait_send()
    for at in over:
        brick_over(*at).wait_send()
    for at in near:
        brick_near(*at).wait_send()
    for n in range(4):
        for copy in brick_far(n // 2, n % 2):
            copy.wait_send()

    def drain(k, carry):
        for copy in (*first_hop(k), *first_share(k), *second_hop(k), *last_share(k), *z_first(k, 0), *z_first(k, 1), *z_second(k)):
            copy.wait_send()
        for b in range(2):
            yr, copy = y_send(b, k)

            @pl.when(y != yr)
            def _():
                copy.wait_send()

        return carry

    lax.fori_loop(0, CHUNKS, drain, 0)


def per_device(snapshots, weights, next_bricks, brick_source):
    rows, width = snapshots.shape
    depth, own = rows // 4, 2 * width
    scale = 1.0 / math.sqrt(rows * lax.axis_size("rows"))
    f32, bf16, dma = jnp.float32, jnp.bfloat16, pltpu.SemaphoreType.DMA
    vmem = pltpu.VMEM
    space = lambda kind: pl.BlockSpec(memory_space=kind)
    count = rows // BRICK
    gram, tiles = pl.pallas_call(
        functools.partial(kernel, scale),
        out_shape=(
            vmem((2 * width, width), f32),
            vmem((count, BRICK, width), f32),
        ),
        in_specs=[space(pl.ANY), space(vmem), space(pl.ANY), space(pltpu.SMEM)],
        out_specs=(space(vmem), space(vmem)),
        scratch_shapes=[
            vmem((2, 4, CHUNKS, depth, LANES), f32),
            vmem((own, 2 * depth), bf16),
            vmem((own, 2 * depth), bf16),
            vmem((2 * depth, 4 * LANES), bf16),
            vmem((2 * depth, 4 * LANES), bf16),
            vmem((CHUNKS, 4, own, LANES), f32),
            vmem((6, CHUNKS, own // 2, LANES), f32),
            vmem((CHUNKS // 2, 3, own // 2, LANES), f32),
            vmem((count, BRICK, width), f32),
            vmem((2, 2, next_bricks.shape[0] // BRICK, BRICK, width), f32),
            vmem((3, 2, next_bricks.shape[0] // BRICK, BRICK, width), f32),
            dma((CHUNKS,)), dma((2, CHUNKS)), dma((2, CHUNKS)), dma((4, CHUNKS)),
            dma((6, CHUNKS)), dma((CHUNKS // 2, 3)), dma((16,)), dma((2, 2)), dma((3, 2)),
            dma((3, 2)), dma((2, CHUNKS)), dma((2, CHUNKS)), dma((4, CHUNKS)),
            dma((6, CHUNKS)), dma((2, CHUNKS)), dma((3,)), dma((2, 2, 2)), dma((3, 2)), dma((2, 2, 2)),
        ],
        compiler_params=pltpu.CompilerParams(
            collective_id=0, has_side_effects=True, vmem_limit_bytes=62464 * 1024
        ),
    )(snapshots, weights.reshape(1, rows), next_bricks.reshape(-1, BRICK, next_bricks.shape[1]), brick_source)
    return gram, tiles.reshape(rows, width)


def solution(mesh):
    return jax.shard_map(
        per_device,
        mesh=mesh,
        in_specs=(P("rows", "snaps"), P("rows"), P(("rows", "snaps"), None), P("rows", None)),
        out_specs=(P("rows", "snaps"), P("rows", "snaps")),
        check_vma=False,
    )
```

```python
import functools
import math

import jax
import jax.numpy as jnp
from jax import lax
from jax.experimental import pallas as pl
from jax.experimental.pallas import tpu as pltpu
from jax.sharding import PartitionSpec as P

BRICK = 32
NX, NZ = 4, 4
CHUNKS = 8
LANES = 128
LAG = 4
MESH = pl.DeviceIdType.MESH


def kernel(
    scale, snap, w_ref, bricks, gram, landed,
    xs, ahi, alo, bhi, blo, ps, zs, ys, relay, across, yin, vs,
    sem_a, sem_x, sem_h, sem_s, sem_z, sem_y, sem_b, sem_r, sem_o, sem_v, sem_w,
    sent,
):
    rb, me = lax.axis_index("rows"), lax.axis_index("snaps")
    z, y_hi = rb // 2, rb % 2
    x, y_lo, c = me // 4, (me // 2) % 2, me % 2
    y = y_hi * 2 + y_lo
    depth = xs.shape[3]
    half = depth // 2

    def snap_of(xx, yl, cc):
        return xx * 4 + yl * 2 + cc

    right = (rb, snap_of((x + 1) % NX, y_lo, c))
    left = (rb, snap_of((x + 3) % NX, y_lo, c))
    twin = (rb, snap_of(x, y_lo, 1 - c))
    up = (((z + 1) % NZ) * 2 + y_hi, me)
    down = (((z + 3) % NZ) * 2 + y_hi, me)

    def round_of(far, part, cc):
        if far == 0:
            return part * 3 + cc
        return 6 + cc if part else 2 + 3 * cc

    def send(src, dst, s_sem, r_sem, to):
        return pltpu.make_async_remote_copy(
            src_ref=src, dst_ref=dst, send_sem=s_sem, recv_sem=r_sem, device_id=to, device_id_type=MESH
        )

    def arrived(dst, sem):
        pltpu.make_async_copy(dst, dst, sem).wait()

    barrier = pltpu.get_barrier_semaphore()
    for o in range(1, 16):
        pl.semaphore_signal(barrier, inc=1, device_id=(rb, (me + o) % 16), device_id_type=MESH)
    pl.semaphore_signal(barrier, inc=1, device_id=up, device_id_type=MESH)
    pl.semaphore_signal(barrier, inc=1, device_id=down, device_id_type=MESH)
    for yl in range(2):
        far = (z * 2 + 1 - y_hi, snap_of(x, yl, c))
        pl.semaphore_signal(barrier, inc=1, device_id=far, device_id_type=MESH)
    pl.semaphore_wait(barrier, 19)

    def reshard(o, part):
        y2, c2 = (y_lo + o // 2) % 2, (c + o % 2) % 2
        q2 = y2 * 2 + c2
        k = round_of(o // 2, part, c)
        src = snap.at[pl.ds(pl.multiple_of(q2 * depth, depth), depth), pl.ds(part * LANES, LANES)]
        dst = xs.at[c2, 0, k]
        if o == 0:
            return pltpu.make_async_copy(src, dst, sem_a.at[k])
        to = (rb, snap_of(x, y2, c2))
        return send(src, dst, sent.at[0], sem_a.at[k], to)

    def brick(o):
        s2 = snap_of(x, (y_lo + o // 2) % 2, (c + o % 2) % 2)
        width = landed.shape[2]
        src = bricks.at[:, :, pl.ds(pl.multiple_of(s2 * width, LANES), width)]
        count = bricks.shape[0]
        dst = landed.at[pl.ds(me * count, count)]
        if o == 0:
            return pltpu.make_async_copy(src, dst, sem_b.at[0])
        return send(src, dst, sent.at[6], sem_b.at[0], (rb, s2))

    def brick_cols(dx, dy, dc):
        width = landed.shape[2]
        s2 = snap_of((x + dx) % NX, (y_lo + dy) % 2, (c + dc) % 2)
        return bricks.at[:, :, pl.ds(pl.multiple_of(s2 * width, LANES), width)]

    def rows_from(source):
        return landed.at[pl.ds(source * bricks.shape[0], bricks.shape[0])]

    def brick_over(dx, dc):
        to = (rb, snap_of(x, 1 - y_lo, c))
        dst = across.at[dx - 1, dc]
        return send(brick_cols(dx, 1, dc), dst, sent.at[6], sem_o.at[0], to)

    def held_bricks(dx, dy, dc):
        return across.at[dx - 1, dc] if dy else brick_cols(dx, 0, dc)

    def brick_near(dx, dy, dc):
        source = snap_of(x, (y_lo + dy) % 2, c)
        to = (rb, snap_of((x + dx) % NX, y_lo, (c + dc) % 2))
        sem = sent.at[7]
        return send(held_bricks(dx, dy, dc), rows_from(source), sem, sem_b.at[0], to)

    def brick_far(g, dy):
        ahead, behind = (x + 1 + 2 * g) % NX, (x + 3 - 2 * g) % NX
        source = snap_of(behind, (y_lo + dy) % 2, c)
        to = (rb, snap_of(ahead, y_lo, (c + g) % 2))
        hop = send(
            held_bricks(2, dy, g), relay.at[g, dy], sent.at[7], sem_r.at[g, dy], left if g else right
        )
        return hop, send(relay.at[g, dy], rows_from(source), sent.at[7], sem_b.at[0], to)

    near = [(dx, dy, dc) for dx in (1, 3) for dy in range(2) for dc in range(2)]
    over = [(dx, dc) for dx in (1, 2, 3) for dc in range(2)]

    for part in range(2):
        for o in (0, 1, 2, 3):
            reshard(o, part).start()
    brick(0).start()
    brick(1).start()

    def first_hop(k):
        return (
            send(xs.at[c, 0, k], xs.at[c, 3, k], sent.at[1], sem_x.at[0, k], right),
            send(xs.at[c, 0, k], xs.at[c, 1, k], sent.at[1], sem_x.at[1, k], left),
        )

    def first_share(k):
        return (send(xs.at[c, 0, k], xs.at[c, 0, k], sent.at[3], sem_s.at[0, k], twin),)

    def second_hop(k):
        lo_rows, hi_rows = pl.ds(0, half), pl.ds(half, half)
        return (
            send(xs.at[c, 3, k, lo_rows], xs.at[c, 2, k, lo_rows], sent.at[2], sem_h.at[k], right),
            send(xs.at[c, 1, k, hi_rows], xs.at[c, 2, k, hi_rows], sent.at[2], sem_h.at[k], left),
            send(xs.at[c, 3, k], xs.at[c, 3, k], sent.at[3], sem_s.at[3, k], twin),
            send(xs.at[c, 1, k], xs.at[c, 1, k], sent.at[3], sem_s.at[1, k], twin),
        )

    def last_share(k):
        return (send(xs.at[c, 2, k], xs.at[c, 2, k], sent.at[3], sem_s.at[2, k], twin),)

    own = ps.shape[2]
    top, bottom = pl.ds(0, own // 2), pl.ds(own // 2, own // 2)

    def slot_of(j):
        return (j - x + 2 * NX) % NX

    def z_send(n, k, j, rows, to):
        return send(ps.at[k, slot_of(j), rows], zs.at[n, k], sent.at[4], sem_z.at[min(n // 2, 1), k], to)

    def z_first(k, b):
        if b == 0:
            return (z_send(0, k, z + 2, top, down), z_send(2, k, z + 1, top, up))
        return (z_send(1, k, z + 2, bottom, up), z_send(3, k, z - 1, bottom, down))

    def z_second(k):
        return (z_send(4, k, z - 1, top, down), z_send(5, k, z + 1, bottom, up))

    def z_add(k, j, rows, ns):
        d = slot_of(j)
        total = ps[k, d, rows]
        for n in ns:
            total = total + zs[n, k]
        ps[k, d, rows] = total

    def y_send(b, k):
        far = k // 5
        h, m = (y_lo + far) % 2, (1 - far) * (k - k // 3) + far * (k - 4)
        yr = h * 2 + b
        slot = (y - yr + 8) % 4 - 1
        rows = top if b == 0 else bottom
        to = (z * 2 + h, snap_of(x, b, c))
        return yr, send(ps.at[k, slot_of(z), rows], ys.at[m, slot], sent.at[5], sem_y.at[m], to)

    def y_first(k, b):
        h = (y_lo + k // 2) % 2
        yr = h * 2 + b
        slot = (y - yr + 8) % 4 - 1
        rows = top if b == 0 else bottom
        to = (z * 2 + h, snap_of(x, b, c))
        return yr, send(ps.at[k, :, rows], yin.at[slot], sent.at[8], sem_v.at[0], to)

    def y_first_go(k):
        for b in range(2):
            yr, copy = y_first(k, b)

            @pl.when(y != yr)
            def _():
                copy.start()

    mine = ((y_hi + y_lo) % 2) * 2
    piece = own // 4

    def v_rows(part):
        return pl.ds(pl.multiple_of(y_lo * (own // 2) + part * piece, piece), piece)

    def v_send(n, j, part, to):
        return send(ps.at[mine, slot_of(j), v_rows(part)], vs.at[n], sent.at[9], sem_w.at[min(n // 2, 1)], to)

    def v_first():
        return (v_send(0, z + 2, 0, down), v_send(1, z + 2, 1, up), v_send(2, z + 1, 0, up), v_send(3, z - 1, 1, down))

    def v_second():
        return (v_send(4, z - 1, 0, down), v_send(5, z + 1, 1, up))

    def v_add(j, part, ns):
        d = slot_of(j)
        total = ps[mine, d, v_rows(part)]
        for n in ns:
            total = total + vs[n]
        ps[mine, d, v_rows(part)] = total

    def issue(copies):
        for copy in copies:
            copy.start()

    def own_operand(far):
        for part in range(2):
            k = round_of(far, part, c)
            at = ((y_lo + far) % 2) * 2 * LANES + part * LANES
            rows = pl.ds(pl.multiple_of(at, LANES), LANES)
            for s in range(2):
                w = w_ref[:, pl.ds(pl.multiple_of(y_lo * 2 * depth + s * depth, LANES), depth)]
                block = xs[s, 0, k].T * (w * scale)
                hi = block.astype(jnp.bfloat16)
                cols = pl.ds(s * depth, depth)
                ahi[rows, cols] = hi
                alo[rows, cols] = (block - hi.astype(jnp.float32)).astype(jnp.bfloat16)

    def split(d, k, at):
        for s in range(2):
            block = xs[s, d, k]
            hi = block.astype(jnp.bfloat16)
            rows, cols = pl.ds(s * depth, depth), pl.ds(at, LANES)
            bhi[rows, cols] = hi
            blo[rows, cols] = (block - hi.astype(jnp.float32)).astype(jnp.bfloat16)

    order_of = (0, 1, 3, 2)

    def product(far, k, k2, first=0, last=4):
        dot = functools.partial(jnp.dot, preferred_element_type=jnp.float32)
        size = own // 2
        rows = pl.ds(pl.multiple_of(((y_lo + far) % 2) * size, size), size)
        cols = pl.ds(first * LANES, (last - first) * LANES)
        a, b = ahi[rows, :], bhi[:, cols]
        out = dot(a, b) + (dot(a, blo[:, cols]) + dot(alo[rows, :], b))
        for n in range(first, last):
            d = order_of[n]
            ps[k2 if d == 2 else k, d, rows] = out[:, (n - first) * LANES : (n - first + 1) * LANES]

    def gathered(n, k):
        d = order_of[n]
        if d:
            arrived(xs.at[1 - c, d, k], sem_s.at[d, k])
        split(d, k, n * LANES)

    def z_go(k, late):
        for b in range(2):
            for j, copy in zip((z + 2, z + 1 - 2 * b), z_first(k, b)):

                @pl.when((slot_of(j) == 2) == late)
                def _():
                    copy.start()

    def early(k):
        for n in range(4):
            gathered(n, k)
        product(0, k, k)
        for b in range(2 if k else 0):

            @pl.when(y_lo == b)
            def _():
                issue(z_first(k, b))

    def pass_on(k):
        arrived(xs.at[c, 3, k], sem_x.at[0, k])
        arrived(xs.at[c, 1, k], sem_x.at[1, k])
        issue(second_hop(k))

    def pass_last(k):
        arrived(xs.at[c, 2, k], sem_h.at[k])
        issue(last_share(k))

    def step(i, carry):
        @pl.when(i + 1 < CHUNKS)
        def _():
            pass_on(i + 1)

        @pl.when(i + 3 < CHUNKS)
        def _():
            issue(first_hop(i + 3))

        @pl.when(i + 1 == CHUNKS - 1)
        def _():
            arrived(across, sem_o.at[0])
            for n in range(4):
                brick_far(n % 2, n // 2)[0].start()
            for at in near:
                brick_near(*at).start()

        @pl.when(i < CHUNKS)
        def _():
            pass_last(i)

        @pl.when(i + 1 < CHUNKS)
        def _():
            for n in range(3):
                gathered(n, i + 1)
            gathered(3, i)
            for far in range(2):
                product(far, i + 1, i)
            @pl.when(i == 2)
            def _():
                y_first_go(2)

            @pl.when(i > 2)
            def _():
                z_go(i, True)

            z_go(i + 1, False)

        @pl.when(i == CHUNKS - 1)
        def _():
            gathered(3, i)
            for far in range(2):
                product(far, i, i, first=3)
            z_go(i, True)

        def z_pass(k):
            arrived(zs.at[pl.ds(0, 2), k], sem_z.at[0, k])
            z_add(k, z - 1, top, (0,))
            z_add(k, z + 1, bottom, (1,))
            issue(z_second(k))

        def z_last(k):
            arrived(zs.at[pl.ds(2, 4), k], sem_z.at[1, k])
            z_add(k, z, top, (2, 4))
            z_add(k, z, bottom, (3, 5))
            for b in range(2):
                yr, copy = y_send(b, k)

                @pl.when(y != yr)
                def _():
                    copy.start()

        @pl.when((i != 3) & (i < CHUNKS + 1))
        def _():
            z_pass(i - 1)

        @pl.when((i == 4) | ((i >= 6) & (i < CHUNKS + 3)))
        def _():
            z_last(i - 3)

        @pl.when(i == CHUNKS - 1)
        def _():
            for n in range(4):
                g, dy = n // 2, n % 2
                arrived(relay.at[g, dy], sem_r.at[g, dy])
                brick_far(g, dy)[1].start()

        @pl.when(i == 7)
        def _():
            arrived(yin, sem_v.at[0])
            rows = pl.ds(pl.multiple_of(y_lo * (own // 2), own // 2), own // 2)
            for d in range(4):
                ps[mine, d, rows] = ps[mine, d, rows] + (yin[0, d] + (yin[1, d] + yin[2, d]))
            issue(v_first())

        @pl.when(i == 8)
        def _():
            arrived(vs.at[pl.ds(0, 2)], sem_w.at[0])
            v_add(z - 1, 0, (0,))
            v_add(z + 1, 1, (1,))
            issue(v_second())

        @pl.when(i == 10)
        def _():
            arrived(vs.at[pl.ds(2, 4)], sem_w.at[1])
            v_add(z, 0, (2, 4))
            v_add(z, 1, (3, 5))
            rows = pl.ds(pl.multiple_of(y_lo * (own // 2), own // 2), own // 2)
            gram[pl.ds(0, LANES), :] = ps[mine, slot_of(z), rows].T

        @pl.when(i >= 5 + LAG)
        def _():
            m = i - 4 - LAG
            far = (y_hi + y_lo) % 2
            k = (1 - far) * (m + m // 2) + far * (m + 4)
            arrived(ys.at[m], sem_y.at[m])
            here = ps[k, slot_of(z), pl.ds(pl.multiple_of(y_lo * (own // 2), own // 2), own // 2)]
            total = here + (ys[m, 0] + (ys[m, 1] + ys[m, 2]))
            at = (m % 2) * 2 * LANES + (m // 2) * LANES
            gram[pl.ds(pl.multiple_of(at, LANES), LANES), :] = total.T

        return carry

    def ready(k):
        arrived(xs.at[c, 0, k], sem_a.at[k])
        issue(first_share(k))

    for k in (0, 1, 3, 4):
        ready(k)
        if k < 2:
            issue(first_hop(k))
    for k in (0, 1, 3, 4):
        arrived(xs.at[1 - c, 0, k], sem_s.at[0, k])
    own_operand(0)
    pass_on(0)
    ready(2)
    issue(first_hop(2))
    pass_on(1)
    issue(first_hop(3))
    pass_last(0)
    ready(5)
    early(0)
    pass_on(2)
    issue(first_hop(4))
    pass_last(1)
    ready(6)
    ready(7)
    early(1)
    brick(2).start()
    brick(3).start()
    for at in over:
        brick_over(*at).start()
    for k in (2, 5, 6, 7):
        arrived(xs.at[1 - c, 0, k], sem_s.at[0, k])
    own_operand(1)
    for k in range(2):
        for n in range(4):
            split(order_of[n], k, n * LANES)
        product(1, k, k)
        if k == 0:
            y_first_go(0)
            continue
        for b in range(2):

            @pl.when(y_lo != b)
            def _():
                issue(z_first(k, b))

    for n in range(3):
        gathered(n, 2)
    for far in range(2):
        product(far, 2, 2, last=3)
    lax.fori_loop(2, CHUNKS + 3, step, 0)
    arrived(landed, sem_b.at[0])

    lax.fori_loop(CHUNKS + 3, CHUNKS + LAG, step, 0)

    all_sent = (
        xs.at[0, 0, pl.ds(0, 6)], xs.at[0, pl.ds(0, 2)], xs.at[0, 0], xs.at[0], zs.at[:, pl.ds(0, 6)],
        zs.at[pl.ds(0, 3), pl.ds(0, 3)], zs.at[pl.ds(0, 3), pl.ds(0, 3)], landed, yin, vs,
    )
    for n, ref in enumerate(all_sent):
        arrived(ref, sent.at[n])


def finish(order, gathered, summed, tiles, gram, sem_t, sem_g):
    for q in range(tiles.shape[0]):
        pltpu.make_async_copy(gathered.at[order[0, q]], tiles.at[q], sem_t).start()
    whole = pltpu.make_async_copy(summed, gram, sem_g)
    whole.start()
    pltpu.make_async_copy(gathered, tiles, sem_t).wait()
    whole.wait()


def per_device(snapshots, weights, next_bricks, brick_source):
    rows, width = snapshots.shape
    depth, own = rows // 4, 2 * width
    scale = 1.0 / math.sqrt(rows * lax.axis_size("rows"))
    f32, bf16, dma = jnp.float32, jnp.bfloat16, pltpu.SemaphoreType.DMA
    vmem = pltpu.VMEM
    space = lambda kind: pl.BlockSpec(memory_space=kind)
    count = rows // BRICK
    summed, landed = pl.pallas_call(
        functools.partial(kernel, scale),
        out_shape=(
            vmem((2 * width, width), f32),
            vmem((count, BRICK, width), f32),
        ),
        in_specs=[space(pl.ANY), space(vmem), space(pl.ANY)],
        out_specs=(space(vmem), space(pl.ANY)),
        scratch_shapes=[
            vmem((2, 4, CHUNKS, depth, LANES), f32),
            vmem((own, 2 * depth), bf16),
            vmem((own, 2 * depth), bf16),
            vmem((2 * depth, 4 * LANES), bf16),
            vmem((2 * depth, 4 * LANES), bf16),
            vmem((CHUNKS, 4, own, LANES), f32),
            vmem((6, CHUNKS, own // 2, LANES), f32),
            vmem((CHUNKS // 2, 3, own // 2, LANES), f32),
            vmem((2, 2, next_bricks.shape[0] // BRICK, BRICK, width), f32),
            vmem((3, 2, next_bricks.shape[0] // BRICK, BRICK, width), f32),
            vmem((3, 4, own // 2, LANES), f32),
            vmem((6, own // 4, LANES), f32),
            dma((CHUNKS,)), dma((2, CHUNKS)), dma((CHUNKS,)), dma((4, CHUNKS)), dma((2, CHUNKS)), dma((4,)),
            dma((1,)), dma((2, 2)), dma((1,)), dma((1,)), dma((2,)), dma((10,)),
        ],
        compiler_params=pltpu.CompilerParams(
            collective_id=0, has_side_effects=True, vmem_limit_bytes=62464 * 1024
        ),
    )(snapshots, weights.reshape(1, rows), next_bricks.reshape(-1, BRICK, next_bricks.shape[1]))
    tiles, gram = pl.pallas_call(
        finish,
        out_shape=(
            jax.ShapeDtypeStruct((count, BRICK, width), f32),
            jax.ShapeDtypeStruct((2 * width, width), f32),
        ),
        in_specs=[space(pltpu.SMEM), space(pl.ANY), space(pl.ANY)],
        out_specs=(space(pl.ANY), space(pl.ANY)),
        scratch_shapes=[dma, dma],
        compiler_params=pltpu.CompilerParams(vmem_limit_bytes=2 * 1024 * 1024),
    )(brick_source, landed, summed)
    return gram, tiles.reshape(rows, width)


def solution(mesh):
    return jax.shard_map(
        per_device,
        mesh=mesh,
        in_specs=(P("rows", "snaps"), P("rows"), P(("rows", "snaps"), None), P("rows", None)),
        out_specs=(P("rows", "snaps"), P("rows", "snaps")),
        check_vma=False,
    )
```

```python
import functools
import math

import jax
import jax.numpy as jnp
from jax import lax
from jax.experimental import pallas as pl
from jax.experimental.pallas import tpu as pltpu
from jax.sharding import PartitionSpec as P

BRICK = 32
NX, NZ = 4, 4
CHUNKS = 8
LANES = 128
LAG = 4
MESH = pl.DeviceIdType.MESH


def kernel(
    scale, snap, w_ref, bricks, gram, landed,
    xs, ahi, alo, bhi, blo, ps, zs, ys, relay, across, yin, vs,
    sem_a, sem_x, sem_h, sem_s, sem_z, sem_y, sem_b, sem_r, sem_o, sem_v, sem_w,
    sent,
):
    rb, me = lax.axis_index("rows"), lax.axis_index("snaps")
    z, y_hi = rb // 2, rb % 2
    x, y_lo, c = me // 4, (me // 2) % 2, me % 2
    y = y_hi * 2 + y_lo
    depth = xs.shape[3]
    half = depth // 2

    def snap_of(xx, yl, cc):
        return xx * 4 + yl * 2 + cc

    right = (rb, snap_of((x + 1) % NX, y_lo, c))
    left = (rb, snap_of((x + 3) % NX, y_lo, c))
    twin = (rb, snap_of(x, y_lo, 1 - c))
    up = (((z + 1) % NZ) * 2 + y_hi, me)
    down = (((z + 3) % NZ) * 2 + y_hi, me)

    def round_of(far, part, cc):
        if far == 0:
            return 3 + cc if part else 1 - cc
        return 6 + cc if part else 2 + 3 * cc

    def send(src, dst, s_sem, r_sem, to):
        return pltpu.make_async_remote_copy(
            src_ref=src, dst_ref=dst, send_sem=s_sem, recv_sem=r_sem, device_id=to, device_id_type=MESH
        )

    def arrived(dst, sem):
        pltpu.make_async_copy(dst, dst, sem).wait()

    def reshard(o, part):
        y2, c2 = (y_lo + o // 2) % 2, (c + o % 2) % 2
        q2 = y2 * 2 + c2
        k = round_of(o // 2, part, c)
        src = snap.at[pl.ds(pl.multiple_of(q2 * depth, depth), depth), pl.ds(part * LANES, LANES)]
        dst = xs.at[c2, 0, k]
        if o == 0:
            return pltpu.make_async_copy(src, dst, sem_a.at[k])
        to = (rb, snap_of(x, y2, c2))
        return send(src, dst, sent.at[0], sem_a.at[k], to)

    def brick(o):
        s2 = snap_of(x, (y_lo + o // 2) % 2, (c + o % 2) % 2)
        width = landed.shape[2]
        src = bricks.at[:, :, pl.ds(pl.multiple_of(s2 * width, LANES), width)]
        count = bricks.shape[0]
        dst = landed.at[pl.ds(me * count, count)]
        if o == 0:
            return pltpu.make_async_copy(src, dst, sem_b.at[0])
        return send(src, dst, sent.at[6], sem_b.at[0], (rb, s2))

    def brick_cols(dx, dy, dc):
        width = landed.shape[2]
        s2 = snap_of((x + dx) % NX, (y_lo + dy) % 2, (c + dc) % 2)
        return bricks.at[:, :, pl.ds(pl.multiple_of(s2 * width, LANES), width)]

    def rows_from(source):
        return landed.at[pl.ds(source * bricks.shape[0], bricks.shape[0])]

    def brick_over(dx, dc):
        to = (rb, snap_of(x, 1 - y_lo, c))
        dst = across.at[dx - 1, dc]
        return send(brick_cols(dx, 1, dc), dst, sent.at[6], sem_o.at[0], to)

    def held_bricks(dx, dy, dc):
        return across.at[dx - 1, dc] if dy else brick_cols(dx, 0, dc)

    def brick_near(dx, dy, dc):
        source = snap_of(x, (y_lo + dy) % 2, c)
        to = (rb, snap_of((x + dx) % NX, y_lo, (c + dc) % 2))
        sem = sent.at[7]
        return send(held_bricks(dx, dy, dc), rows_from(source), sem, sem_b.at[0], to)

    def brick_far(g, dy):
        ahead, behind = (x + 1 + 2 * g) % NX, (x + 3 - 2 * g) % NX
        source = snap_of(behind, (y_lo + dy) % 2, c)
        to = (rb, snap_of(ahead, y_lo, (c + g) % 2))
        hop = send(
            held_bricks(2, dy, g), relay.at[g, dy], sent.at[7], sem_r.at[g, dy], left if g else right
        )
        return hop, send(relay.at[g, dy], rows_from(source), sent.at[7], sem_b.at[0], to)

    near = [(dx, dy, dc) for dx in (1, 3) for dy in range(2) for dc in range(2)]
    over = [(dx, dc) for dx in (1, 2, 3) for dc in range(2)]

    for part in range(2):
        reshard(0, part).start()
    brick(0).start()

    barrier = pltpu.get_barrier_semaphore()
    for o in range(1, 16):
        pl.semaphore_signal(barrier, inc=1, device_id=(rb, (me + o) % 16), device_id_type=MESH)
    pl.semaphore_signal(barrier, inc=1, device_id=up, device_id_type=MESH)
    pl.semaphore_signal(barrier, inc=1, device_id=down, device_id_type=MESH)
    for yl in range(2):
        far = (z * 2 + 1 - y_hi, snap_of(x, yl, c))
        pl.semaphore_signal(barrier, inc=1, device_id=far, device_id_type=MESH)
    pl.semaphore_wait(barrier, 19)

    for part in range(2):
        for o in (1, 2, 3):
            reshard(o, part).start()
    brick(1).start()

    def first_hop(k):
        return (
            send(xs.at[c, 0, k], xs.at[c, 3, k], sent.at[1], sem_x.at[0, k], right),
            send(xs.at[c, 0, k], xs.at[c, 1, k], sent.at[1], sem_x.at[1, k], left),
        )

    def first_share(k):
        return (send(xs.at[c, 0, k], xs.at[c, 0, k], sent.at[3], sem_s.at[0, k], twin),)

    def second_hop(k):
        lo_rows, hi_rows = pl.ds(0, half), pl.ds(half, half)
        return (
            send(xs.at[c, 3, k, lo_rows], xs.at[c, 2, k, lo_rows], sent.at[2], sem_h.at[k], right),
            send(xs.at[c, 1, k, hi_rows], xs.at[c, 2, k, hi_rows], sent.at[2], sem_h.at[k], left),
            send(xs.at[c, 3, k], xs.at[c, 3, k], sent.at[3], sem_s.at[3, k], twin),
            send(xs.at[c, 1, k], xs.at[c, 1, k], sent.at[3], sem_s.at[1, k], twin),
        )

    def last_share(k):
        return (send(xs.at[c, 2, k], xs.at[c, 2, k], sent.at[3], sem_s.at[2, k], twin),)

    own = ps.shape[2]
    top, bottom = pl.ds(0, own // 2), pl.ds(own // 2, own // 2)

    def slot_of(j):
        return (j - x + 2 * NX) % NX

    def z_send(n, k, j, rows, to):
        return send(ps.at[k, slot_of(j), rows], zs.at[n, k], sent.at[4], sem_z.at[min(n // 2, 1), k], to)

    def z_first(k, b):
        if b == 0:
            return (z_send(0, k, z + 2, top, down), z_send(2, k, z + 1, top, up))
        return (z_send(1, k, z + 2, bottom, up), z_send(3, k, z - 1, bottom, down))

    def z_second(k):
        return (z_send(4, k, z - 1, top, down), z_send(5, k, z + 1, bottom, up))

    def z_add(k, j, rows, ns):
        d = slot_of(j)
        total = ps[k, d, rows]
        for n in ns:
            total = total + zs[n, k]
        ps[k, d, rows] = total

    def y_send(b, k):
        far = k // 5
        h, m = (y_lo + far) % 2, (1 - far) * ((k + 2) // 2) + far * (k - 4)
        yr = h * 2 + b
        slot = (y - yr + 8) % 4 - 1
        rows = top if b == 0 else bottom
        to = (z * 2 + h, snap_of(x, b, c))
        return yr, send(ps.at[k, slot_of(z), rows], ys.at[m, slot], sent.at[5], sem_y.at[m], to)

    def y_first(k, b):
        h = (y_lo + k - 1) % 2
        yr = h * 2 + b
        slot = (y - yr + 8) % 4 - 1
        rows = top if b == 0 else bottom
        to = (z * 2 + h, snap_of(x, b, c))
        return yr, send(ps.at[k, :, rows], yin.at[slot], sent.at[8], sem_v.at[0], to)

    def y_first_go(k):
        for b in range(2):
            yr, copy = y_first(k, b)

            @pl.when(y != yr)
            def _():
                copy.start()

    mine = 1 + (y_hi + y_lo) % 2
    piece = own // 4

    def v_rows(part):
        return pl.ds(pl.multiple_of(y_lo * (own // 2) + part * piece, piece), piece)

    def v_send(n, j, part, to):
        return send(ps.at[mine, slot_of(j), v_rows(part)], vs.at[n], sent.at[9], sem_w.at[min(n // 2, 1)], to)

    def v_first():
        return (v_send(0, z + 2, 0, down), v_send(1, z + 2, 1, up), v_send(2, z + 1, 0, up), v_send(3, z - 1, 1, down))

    def v_second():
        return (v_send(4, z - 1, 0, down), v_send(5, z + 1, 1, up))

    def v_add(j, part, ns):
        d = slot_of(j)
        total = ps[mine, d, v_rows(part)]
        for n in ns:
            total = total + vs[n]
        ps[mine, d, v_rows(part)] = total

    def issue(copies):
        for copy in copies:
            copy.start()

    def own_operand(far):
        for part in range(2):
            k = round_of(far, part, c)
            at = ((y_lo + far) % 2) * 2 * LANES + part * LANES
            rows = pl.ds(pl.multiple_of(at, LANES), LANES)
            for s in range(2):
                w = w_ref[:, pl.ds(pl.multiple_of(y_lo * 2 * depth + s * depth, LANES), depth)]
                block = xs[s, 0, k].T * (w * scale)
                hi = block.astype(jnp.bfloat16)
                cols = pl.ds(s * depth, depth)
                ahi[rows, cols] = hi
                alo[rows, cols] = (block - hi.astype(jnp.float32)).astype(jnp.bfloat16)

    def split(d, k, at):
        for s in range(2):
            block = xs[s, d, k]
            hi = block.astype(jnp.bfloat16)
            rows, cols = pl.ds(s * depth, depth), pl.ds(at, LANES)
            bhi[rows, cols] = hi
            blo[rows, cols] = (block - hi.astype(jnp.float32)).astype(jnp.bfloat16)

    order_of = (0, 1, 3, 2)

    def product(far, k, k2, first=0, last=4):
        dot = functools.partial(jnp.dot, preferred_element_type=jnp.float32)
        size = own // 2
        rows = pl.ds(pl.multiple_of(((y_lo + far) % 2) * size, size), size)
        cols = pl.ds(first * LANES, (last - first) * LANES)
        a, b = ahi[rows, :], bhi[:, cols]
        out = dot(a, b) + (dot(a, blo[:, cols]) + dot(alo[rows, :], b))
        for n in range(first, last):
            d = order_of[n]
            ps[k2 if d == 2 else k, d, rows] = out[:, (n - first) * LANES : (n - first + 1) * LANES]

    def gathered(n, k):
        d = order_of[n]
        if d:
            arrived(xs.at[1 - c, d, k], sem_s.at[d, k])
        split(d, k, n * LANES)

    def z_go(k, late):
        for b in range(2):
            for j, copy in zip((z + 2, z + 1 - 2 * b), z_first(k, b)):

                @pl.when((slot_of(j) == 2) == late)
                def _():
                    copy.start()

    def early(k):
        for n in range(4):
            gathered(n, k)
        product(0, k, k)
        for b in range(0 if k else 2):

            @pl.when(y_lo == b)
            def _():
                issue(z_first(k, b))

    def pass_on(k):
        arrived(xs.at[c, 3, k], sem_x.at[0, k])
        arrived(xs.at[c, 1, k], sem_x.at[1, k])
        issue(second_hop(k))

    def pass_last(k):
        arrived(xs.at[c, 2, k], sem_h.at[k])
        issue(last_share(k))

    def step(i, carry):
        @pl.when(i + 1 < CHUNKS)
        def _():
            pass_on(i + 1)

        @pl.when(i + 3 < CHUNKS)
        def _():
            issue(first_hop(i + 3))

        @pl.when(i + 1 == CHUNKS - 1)
        def _():
            arrived(across, sem_o.at[0])
            for n in range(4):
                brick_far(n % 2, n // 2)[0].start()
            for at in near:
                brick_near(*at).start()

        @pl.when(i < CHUNKS)
        def _():
            pass_last(i)

        @pl.when(i + 1 < CHUNKS)
        def _():
            for n in range(3):
                gathered(n, i + 1)
            gathered(3, i)
            for far in range(2):
                product(far, i + 1, i)
            @pl.when(i == 2)
            def _():
                y_first_go(2)

            @pl.when(i > 2)
            def _():
                z_go(i, True)

            z_go(i + 1, False)

        @pl.when(i == CHUNKS - 1)
        def _():
            gathered(3, i)
            for far in range(2):
                product(far, i, i, first=3)
            z_go(i, True)

        def z_pass(k):
            arrived(zs.at[pl.ds(0, 2), k], sem_z.at[0, k])
            z_add(k, z - 1, top, (0,))
            z_add(k, z + 1, bottom, (1,))
            issue(z_second(k))

        def z_last(k):
            arrived(zs.at[pl.ds(2, 4), k], sem_z.at[1, k])
            z_add(k, z, top, (2, 4))
            z_add(k, z, bottom, (3, 5))
            for b in range(2):
                yr, copy = y_send(b, k)

                @pl.when(y != yr)
                def _():
                    copy.start()

        @pl.when(i == 2)
        def _():
            z_pass(0)

        @pl.when((i >= 4) & (i < CHUNKS + 1))
        def _():
            z_pass(i - 1)

        @pl.when(i == 8)
        def _():
            arrived(yin, sem_v.at[0])
            rows = pl.ds(pl.multiple_of(y_lo * (own // 2), own // 2), own // 2)
            for d in range(4):
                ps[mine, d, rows] = ps[mine, d, rows] + (yin[0, d] + (yin[1, d] + yin[2, d]))
            issue(v_first())

        @pl.when(i == 4)
        def _():
            z_last(0)

        @pl.when((i >= 6) & (i < CHUNKS + 3))
        def _():
            z_last(i - 3)

        @pl.when(i == CHUNKS - 1)
        def _():
            for n in range(4):
                g, dy = n // 2, n % 2
                arrived(relay.at[g, dy], sem_r.at[g, dy])
                brick_far(g, dy)[1].start()

        @pl.when(i == 10)
        def _():
            arrived(vs.at[pl.ds(0, 2)], sem_w.at[0])
            v_add(z - 1, 0, (0,))
            v_add(z + 1, 1, (1,))
            issue(v_second())

        @pl.when(i == 11)
        def _():
            arrived(vs.at[pl.ds(2, 4)], sem_w.at[1])
            v_add(z, 0, (2, 4))
            v_add(z, 1, (3, 5))
            rows = pl.ds(pl.multiple_of(y_lo * (own // 2), own // 2), own // 2)
            gram[pl.ds(0, LANES), :] = ps[mine, slot_of(z), rows].T

        @pl.when(i >= 5 + LAG)
        def _():
            m = i - 4 - LAG
            far = (y_hi + y_lo) % 2
            k = (1 - far) * (m + m // 2 - (3 - m) // 2) + far * (m + 4)
            arrived(ys.at[m], sem_y.at[m])
            here = ps[k, slot_of(z), pl.ds(pl.multiple_of(y_lo * (own // 2), own // 2), own // 2)]
            total = here + (ys[m, 0] + (ys[m, 1] + ys[m, 2]))
            at = (m % 2) * 2 * LANES + (m // 2) * LANES
            gram[pl.ds(pl.multiple_of(at, LANES), LANES), :] = total.T

        return carry

    def ready(k):
        arrived(xs.at[c, 0, k], sem_a.at[k])
        issue(first_share(k))

    for k in (0, 1, 3, 4):
        ready(k)
        if k < 2:
            issue(first_hop(k))
    for k in (0, 1, 3, 4):
        arrived(xs.at[1 - c, 0, k], sem_s.at[0, k])
    own_operand(0)
    pass_on(0)
    ready(2)
    issue(first_hop(2))
    pass_on(1)
    issue(first_hop(3))
    pass_last(0)
    ready(5)
    early(0)
    pass_on(2)
    issue(first_hop(4))
    pass_last(1)
    ready(6)
    ready(7)
    early(1)
    brick(2).start()
    brick(3).start()
    for at in over:
        brick_over(*at).start()
    for k in (2, 5, 6, 7):
        arrived(xs.at[1 - c, 0, k], sem_s.at[0, k])
    own_operand(1)
    for k in range(2):
        for n in range(4):
            split(order_of[n], k, n * LANES)
        product(1, k, k)
        if k == 1:
            y_first_go(1)
            continue
        for b in range(2):

            @pl.when(y_lo != b)
            def _():
                issue(z_first(k, b))

    for n in range(3):
        gathered(n, 2)
    for far in range(2):
        product(far, 2, 2, last=3)
    lax.fori_loop(2, CHUNKS + 3, step, 0)
    arrived(landed, sem_b.at[0])

    lax.fori_loop(CHUNKS + 3, CHUNKS + LAG, step, 0)

    all_sent = (
        xs.at[0, 0, pl.ds(0, 6)], xs.at[0, pl.ds(0, 2)], xs.at[0, 0], xs.at[0], zs.at[:, pl.ds(0, 6)],
        zs.at[pl.ds(0, 3), pl.ds(0, 3)], zs.at[pl.ds(0, 3), pl.ds(0, 3)], landed, yin, vs,
    )
    for n, ref in enumerate(all_sent):
        arrived(ref, sent.at[n])


def finish(order, gathered, summed, tiles, gram, sem_t, sem_g):
    for q in range(tiles.shape[0]):
        pltpu.make_async_copy(gathered.at[order[0, q]], tiles.at[q], sem_t).start()
    whole = pltpu.make_async_copy(summed, gram, sem_g)
    whole.start()
    pltpu.make_async_copy(gathered, tiles, sem_t).wait()
    whole.wait()


def per_device(snapshots, weights, next_bricks, brick_source):
    rows, width = snapshots.shape
    depth, own = rows // 4, 2 * width
    scale = 1.0 / math.sqrt(rows * lax.axis_size("rows"))
    f32, bf16, dma = jnp.float32, jnp.bfloat16, pltpu.SemaphoreType.DMA
    vmem = pltpu.VMEM
    space = lambda kind: pl.BlockSpec(memory_space=kind)
    count = rows // BRICK
    summed, landed = pl.pallas_call(
        functools.partial(kernel, scale),
        out_shape=(
            vmem((2 * width, width), f32),
            vmem((count, BRICK, width), f32),
        ),
        in_specs=[space(pl.ANY), space(vmem), space(pl.ANY)],
        out_specs=(space(vmem), space(pl.ANY)),
        scratch_shapes=[
            vmem((2, 4, CHUNKS, depth, LANES), f32),
            vmem((own, 2 * depth), bf16),
            vmem((own, 2 * depth), bf16),
            vmem((2 * depth, 4 * LANES), bf16),
            vmem((2 * depth, 4 * LANES), bf16),
            vmem((CHUNKS, 4, own, LANES), f32),
            vmem((6, CHUNKS, own // 2, LANES), f32),
            vmem((CHUNKS // 2, 3, own // 2, LANES), f32),
            vmem((2, 2, next_bricks.shape[0] // BRICK, BRICK, width), f32),
            vmem((3, 2, next_bricks.shape[0] // BRICK, BRICK, width), f32),
            vmem((3, 4, own // 2, LANES), f32),
            vmem((6, own // 4, LANES), f32),
            dma((CHUNKS,)), dma((2, CHUNKS)), dma((CHUNKS,)), dma((4, CHUNKS)), dma((2, CHUNKS)), dma((4,)),
            dma((1,)), dma((2, 2)), dma((1,)), dma((1,)), dma((2,)), dma((10,)),
        ],
        compiler_params=pltpu.CompilerParams(
            collective_id=0, has_side_effects=True, vmem_limit_bytes=62464 * 1024
        ),
    )(snapshots, weights.reshape(1, rows), next_bricks.reshape(-1, BRICK, next_bricks.shape[1]))
    tiles, gram = pl.pallas_call(
        finish,
        out_shape=(
            jax.ShapeDtypeStruct((count, BRICK, width), f32),
            jax.ShapeDtypeStruct((2 * width, width), f32),
        ),
        in_specs=[space(pltpu.SMEM), space(pl.ANY), space(pl.ANY)],
        out_specs=(space(pl.ANY), space(pl.ANY)),
        scratch_shapes=[dma, dma],
        compiler_params=pltpu.CompilerParams(vmem_limit_bytes=2 * 1024 * 1024),
    )(brick_source, landed, summed)
    return gram, tiles.reshape(rows, width)


def solution(mesh):
    return jax.shard_map(
        per_device,
        mesh=mesh,
        in_specs=(P("rows", "snaps"), P("rows"), P(("rows", "snaps"), None), P("rows", None)),
        out_specs=(P("rows", "snaps"), P("rows", "snaps")),
        check_vma=False,
    )
```

```python
import functools
import math

import jax
import jax.numpy as jnp
from jax import lax
from jax.experimental import pallas as pl
from jax.experimental.pallas import tpu as pltpu
from jax.sharding import PartitionSpec as P

BRICK = 32
NX, NZ = 4, 4
CHUNKS = 8
LANES = 128
LAG = 4
MESH = pl.DeviceIdType.MESH


def kernel(
    scale, snap, weights, bricks, gram, landed,
    w_ref, xs, ahi, alo, bhi, blo, ps, zs, ys, relay, across, yin, vs,
    sem_a, sem_x, sem_h, sem_s, sem_z, sem_y, sem_b, sem_r, sem_o, sem_v, sem_w, sem_c,
    sent,
):
    rb, me = lax.axis_index("rows"), lax.axis_index("snaps")
    z, y_hi = rb // 2, rb % 2
    x, y_lo, c = me // 4, (me // 2) % 2, me % 2
    y = y_hi * 2 + y_lo
    depth = xs.shape[3]
    half = depth // 2

    def snap_of(xx, yl, cc):
        return xx * 4 + yl * 2 + cc

    right = (rb, snap_of((x + 1) % NX, y_lo, c))
    left = (rb, snap_of((x + 3) % NX, y_lo, c))
    twin = (rb, snap_of(x, y_lo, 1 - c))
    up = (((z + 1) % NZ) * 2 + y_hi, me)
    down = (((z + 3) % NZ) * 2 + y_hi, me)

    def round_of(far, part, cc):
        if far == 0:
            return 3 + cc if part else 1 - cc
        return 6 + cc if part else 2 + 3 * cc

    def send(src, dst, s_sem, r_sem, to):
        return pltpu.make_async_remote_copy(
            src_ref=src, dst_ref=dst, send_sem=s_sem, recv_sem=r_sem, device_id=to, device_id_type=MESH
        )

    def arrived(dst, sem):
        pltpu.make_async_copy(dst, dst, sem).wait()

    def reshard(o, part):
        y2, c2 = (y_lo + o // 2) % 2, (c + o % 2) % 2
        q2 = y2 * 2 + c2
        k = round_of(o // 2, part, c)
        src = snap.at[pl.ds(pl.multiple_of(q2 * depth, depth), depth), pl.ds(part * LANES, LANES)]
        dst = xs.at[c2, 0, k]
        if o == 0:
            return pltpu.make_async_copy(src, dst, sem_a.at[k])
        to = (rb, snap_of(x, y2, c2))
        return send(src, dst, sent.at[0], sem_a.at[k], to)

    def brick(o):
        s2 = snap_of(x, (y_lo + o // 2) % 2, (c + o % 2) % 2)
        width = landed.shape[2]
        src = bricks.at[:, :, pl.ds(pl.multiple_of(s2 * width, LANES), width)]
        count = bricks.shape[0]
        dst = landed.at[pl.ds(me * count, count)]
        if o == 0:
            return pltpu.make_async_copy(src, dst, sem_b.at[0])
        return send(src, dst, sent.at[6], sem_b.at[0], (rb, s2))

    def brick_cols(dx, dy, dc):
        width = landed.shape[2]
        s2 = snap_of((x + dx) % NX, (y_lo + dy) % 2, (c + dc) % 2)
        return bricks.at[:, :, pl.ds(pl.multiple_of(s2 * width, LANES), width)]

    def rows_from(source):
        return landed.at[pl.ds(source * bricks.shape[0], bricks.shape[0])]

    def brick_over(dx, dc):
        to = (rb, snap_of(x, 1 - y_lo, c))
        dst = across.at[dx - 1, dc]
        return send(brick_cols(dx, 1, dc), dst, sent.at[6], sem_o.at[0], to)

    def held_bricks(dx, dy, dc):
        return across.at[dx - 1, dc] if dy else brick_cols(dx, 0, dc)

    def brick_near(dx, dy, dc):
        source = snap_of(x, (y_lo + dy) % 2, c)
        to = (rb, snap_of((x + dx) % NX, y_lo, (c + dc) % 2))
        sem = sent.at[7]
        return send(held_bricks(dx, dy, dc), rows_from(source), sem, sem_b.at[0], to)

    def brick_far(g, dy):
        ahead, behind = (x + 1 + 2 * g) % NX, (x + 3 - 2 * g) % NX
        source = snap_of(behind, (y_lo + dy) % 2, c)
        to = (rb, snap_of(ahead, y_lo, (c + g) % 2))
        hop = send(
            held_bricks(2, dy, g), relay.at[g, dy], sent.at[7], sem_r.at[g, dy], left if g else right
        )
        return hop, send(relay.at[g, dy], rows_from(source), sent.at[7], sem_b.at[0], to)

    near = [(dx, dy, dc) for dx in (1, 3) for dy in range(2) for dc in range(2)]
    over = [(dx, dc) for dx in (1, 2, 3) for dc in range(2)]

    w_copy = pltpu.make_async_copy(weights, w_ref, sem_c)
    w_copy.start()
    for part in range(2):
        reshard(0, part).start()
    brick(0).start()

    barrier = pltpu.get_barrier_semaphore()
    for o in range(1, 16):
        pl.semaphore_signal(barrier, inc=1, device_id=(rb, (me + o) % 16), device_id_type=MESH)
    pl.semaphore_signal(barrier, inc=1, device_id=up, device_id_type=MESH)
    pl.semaphore_signal(barrier, inc=1, device_id=down, device_id_type=MESH)
    for yl in range(2):
        far = (z * 2 + 1 - y_hi, snap_of(x, yl, c))
        pl.semaphore_signal(barrier, inc=1, device_id=far, device_id_type=MESH)
    pl.semaphore_wait(barrier, 19)

    for part in range(2):
        for o in (1, 2, 3):
            reshard(o, part).start()
    brick(1).start()

    def first_hop(k):
        return (
            send(xs.at[c, 0, k], xs.at[c, 3, k], sent.at[1], sem_x.at[0, k], right),
            send(xs.at[c, 0, k], xs.at[c, 1, k], sent.at[1], sem_x.at[1, k], left),
        )

    def first_share(k):
        return (send(xs.at[c, 0, k], xs.at[c, 0, k], sent.at[3], sem_s.at[0, k], twin),)

    def second_hop(k):
        lo_rows, hi_rows = pl.ds(0, half), pl.ds(half, half)
        return (
            send(xs.at[c, 3, k, lo_rows], xs.at[c, 2, k, lo_rows], sent.at[2], sem_h.at[k], right),
            send(xs.at[c, 1, k, hi_rows], xs.at[c, 2, k, hi_rows], sent.at[2], sem_h.at[k], left),
            send(xs.at[c, 3, k], xs.at[c, 3, k], sent.at[3], sem_s.at[3, k], twin),
            send(xs.at[c, 1, k], xs.at[c, 1, k], sent.at[3], sem_s.at[1, k], twin),
        )

    def last_share(k):
        return (send(xs.at[c, 2, k], xs.at[c, 2, k], sent.at[3], sem_s.at[2, k], twin),)

    own = ps.shape[2]
    top, bottom = pl.ds(0, own // 2), pl.ds(own // 2, own // 2)

    def slot_of(j):
        return (j - x + 2 * NX) % NX

    def z_send(n, k, j, rows, to):
        return send(ps.at[k, slot_of(j), rows], zs.at[n, k], sent.at[4], sem_z.at[min(n // 2, 1), k], to)

    def z_first(k, b):
        if b == 0:
            return (z_send(0, k, z + 2, top, down), z_send(2, k, z + 1, top, up))
        return (z_send(1, k, z + 2, bottom, up), z_send(3, k, z - 1, bottom, down))

    def z_second(k):
        return (z_send(4, k, z - 1, top, down), z_send(5, k, z + 1, bottom, up))

    def z_add(k, j, rows, ns):
        d = slot_of(j)
        total = ps[k, d, rows]
        for n in ns:
            total = total + zs[n, k]
        ps[k, d, rows] = total

    def y_send(b, k):
        far = k // 5
        h, m = (y_lo + far) % 2, (1 - far) * ((k + 2) // 2) + far * (k - 4)
        yr = h * 2 + b
        slot = (y - yr + 8) % 4 - 1
        rows = top if b == 0 else bottom
        to = (z * 2 + h, snap_of(x, b, c))
        return yr, send(ps.at[k, slot_of(z), rows], ys.at[m, slot], sent.at[5], sem_y.at[m], to)

    def y_first(k, b):
        h = (y_lo + k - 1) % 2
        yr = h * 2 + b
        slot = (y - yr + 8) % 4 - 1
        rows = top if b == 0 else bottom
        to = (z * 2 + h, snap_of(x, b, c))
        return yr, send(ps.at[k, :, rows], yin.at[slot], sent.at[8], sem_v.at[0], to)

    def y_first_go(k):
        for b in range(2):
            yr, copy = y_first(k, b)

            @pl.when(y != yr)
            def _():
                copy.start()

    mine = 1 + (y_hi + y_lo) % 2
    piece = own // 4

    def v_rows(part):
        return pl.ds(pl.multiple_of(y_lo * (own // 2) + part * piece, piece), piece)

    def v_send(n, j, part, to):
        return send(ps.at[mine, slot_of(j), v_rows(part)], vs.at[n], sent.at[9], sem_w.at[min(n // 2, 1)], to)

    def v_first():
        return (v_send(0, z + 2, 0, down), v_send(1, z + 2, 1, up), v_send(2, z + 1, 0, up), v_send(3, z - 1, 1, down))

    def v_second():
        return (v_send(4, z - 1, 0, down), v_send(5, z + 1, 1, up))

    def v_add(j, part, ns):
        d = slot_of(j)
        total = ps[mine, d, v_rows(part)]
        for n in ns:
            total = total + vs[n]
        ps[mine, d, v_rows(part)] = total

    def issue(copies):
        for copy in copies:
            copy.start()

    def own_operand(far):
        for part in range(2):
            k = round_of(far, part, c)
            at = ((y_lo + far) % 2) * 2 * LANES + part * LANES
            rows = pl.ds(pl.multiple_of(at, LANES), LANES)
            for s in range(2):
                w = w_ref[:, pl.ds(pl.multiple_of(y_lo * 2 * depth + s * depth, LANES), depth)]
                block = xs[s, 0, k].T * (w * scale)
                hi = block.astype(jnp.bfloat16)
                cols = pl.ds(s * depth, depth)
                ahi[rows, cols] = hi
                alo[rows, cols] = (block - hi.astype(jnp.float32)).astype(jnp.bfloat16)

    def split(d, k, at):
        for s in range(2):
            block = xs[s, d, k]
            hi = block.astype(jnp.bfloat16)
            rows, cols = pl.ds(s * depth, depth), pl.ds(at, LANES)
            bhi[rows, cols] = hi
            blo[rows, cols] = (block - hi.astype(jnp.float32)).astype(jnp.bfloat16)

    order_of = (0, 1, 3, 2)

    def product(far, k, k2, first=0, last=4):
        dot = functools.partial(jnp.dot, preferred_element_type=jnp.float32)
        size = own // 2
        rows = pl.ds(pl.multiple_of(((y_lo + far) % 2) * size, size), size)
        cols = pl.ds(first * LANES, (last - first) * LANES)
        a, b = ahi[rows, :], bhi[:, cols]
        out = dot(a, b) + (dot(a, blo[:, cols]) + dot(alo[rows, :], b))
        for n in range(first, last):
            d = order_of[n]
            ps[k2 if d == 2 else k, d, rows] = out[:, (n - first) * LANES : (n - first + 1) * LANES]

    def gathered(n, k):
        d = order_of[n]
        if d:
            arrived(xs.at[1 - c, d, k], sem_s.at[d, k])
        split(d, k, n * LANES)

    def z_go(k, late, direct):
        for b in range(2):
            j = z + 1 - 2 * b if direct else z + 2
            copy = z_first(k, b)[direct]

            @pl.when((slot_of(j) == 2) == late)
            def _():
                copy.start()

    def early(k):
        for n in range(4):
            gathered(n, k)
        product(0, k, k)
        for b in range(0 if k else 2):

            @pl.when(y_lo == b)
            def _():
                issue(z_first(k, b))

    def pass_on(k):
        arrived(xs.at[c, 3, k], sem_x.at[0, k])
        arrived(xs.at[c, 1, k], sem_x.at[1, k])
        issue(second_hop(k))

    def pass_last(k):
        arrived(xs.at[c, 2, k], sem_h.at[k])
        issue(last_share(k))

    def step(i, carry):
        @pl.when(i + 1 < CHUNKS)
        def _():
            pass_on(i + 1)

        @pl.when(i + 3 < CHUNKS)
        def _():
            issue(first_hop(i + 3))

        @pl.when(i + 1 == CHUNKS - 1)
        def _():
            arrived(across, sem_o.at[0])
            for n in range(4):
                brick_far(n % 2, n // 2)[0].start()
            for at in near:
                brick_near(*at).start()

        @pl.when(i < CHUNKS)
        def _():
            pass_last(i)

        def z_pass(k):
            arrived(zs.at[pl.ds(0, 2), k], sem_z.at[0, k])
            z_add(k, z - 1, top, (0,))
            z_add(k, z + 1, bottom, (1,))
            issue(z_second(k))

        def z_last(k):
            arrived(zs.at[pl.ds(2, 4), k], sem_z.at[1, k])
            z_add(k, z, top, (2, 4))
            z_add(k, z, bottom, (3, 5))
            for b in range(2):
                yr, copy = y_send(b, k)

                @pl.when(y != yr)
                def _():
                    copy.start()

        @pl.when((i >= 4) & (i <= 6))
        def _():
            z_pass(i - 1)

        @pl.when(i + 1 < CHUNKS)
        def _():
            for n in range(3):
                gathered(n, i + 1)
            gathered(3, i)
            for far in range(2):
                product(far, i + 1, i)
            @pl.when(i == 2)
            def _():
                y_first_go(2)

            @pl.when(i > 2)
            def _():
                z_go(i, True, 0)

            z_go(i + 1, False, 0)

            @pl.when(i > 2)
            def _():
                z_go(i, True, 1)

            @pl.when(i + 1 < CHUNKS - 1)
            def _():
                z_go(i + 1, False, 1)

        @pl.when(i == CHUNKS - 1)
        def _():
            gathered(3, i)
            for far in range(2):
                product(far, i, i, first=3)
            z_go(i, True, 0)
            z_pass(i - 1)
            for b in range(2):
                z_first(i, b)[1].start()

        @pl.when(i == 2)
        def _():
            z_pass(0)

        @pl.when(i == CHUNKS)
        def _():
            z_pass(i - 1)

        @pl.when(i == 8)
        def _():
            arrived(yin, sem_v.at[0])
            rows = pl.ds(pl.multiple_of(y_lo * (own // 2), own // 2), own // 2)
            for d in range(4):
                ps[mine, d, rows] = ps[mine, d, rows] + (yin[0, d] + (yin[1, d] + yin[2, d]))
            issue(v_first())

        @pl.when(i == 4)
        def _():
            z_last(0)

        @pl.when((i >= 6) & (i < CHUNKS + 3))
        def _():
            z_last(i - 3)

        @pl.when(i == CHUNKS - 1)
        def _():
            for n in range(4):
                g, dy = n // 2, n % 2
                arrived(relay.at[g, dy], sem_r.at[g, dy])
                brick_far(g, dy)[1].start()

        @pl.when(i == 10)
        def _():
            arrived(vs.at[pl.ds(0, 2)], sem_w.at[0])
            v_add(z - 1, 0, (0,))
            v_add(z + 1, 1, (1,))
            issue(v_second())

        @pl.when(i == 11)
        def _():
            arrived(vs.at[pl.ds(2, 4)], sem_w.at[1])
            v_add(z, 0, (2, 4))
            v_add(z, 1, (3, 5))
            rows = pl.ds(pl.multiple_of(y_lo * (own // 2), own // 2), own // 2)
            gram[pl.ds(0, LANES), :] = ps[mine, slot_of(z), rows].T

        @pl.when(i >= 5 + LAG)
        def _():
            m = i - 4 - LAG
            far = (y_hi + y_lo) % 2
            k = (1 - far) * (m + m // 2 - (3 - m) // 2) + far * (m + 4)
            arrived(ys.at[m], sem_y.at[m])
            here = ps[k, slot_of(z), pl.ds(pl.multiple_of(y_lo * (own // 2), own // 2), own // 2)]
            total = here + (ys[m, 0] + (ys[m, 1] + ys[m, 2]))
            at = (m % 2) * 2 * LANES + (m // 2) * LANES
            gram[pl.ds(pl.multiple_of(at, LANES), LANES), :] = total.T

        return carry

    def ready(k):
        arrived(xs.at[c, 0, k], sem_a.at[k])
        issue(first_share(k))

    for k in (0, 1, 3, 4):
        ready(k)
        if k < 2:
            issue(first_hop(k))
    for k in (0, 1, 3, 4):
        arrived(xs.at[1 - c, 0, k], sem_s.at[0, k])
    w_copy.wait()
    own_operand(0)
    pass_on(0)
    ready(2)
    issue(first_hop(2))
    pass_on(1)
    issue(first_hop(3))
    pass_last(0)
    ready(5)
    early(0)
    pass_on(2)
    issue(first_hop(4))
    pass_last(1)
    ready(6)
    ready(7)
    early(1)
    brick(2).start()
    brick(3).start()
    for at in over:
        brick_over(*at).start()
    for k in (2, 5, 6, 7):
        arrived(xs.at[1 - c, 0, k], sem_s.at[0, k])
    own_operand(1)
    for k in range(2):
        for n in range(4):
            split(order_of[n], k, n * LANES)
        product(1, k, k)
        if k == 1:
            y_first_go(1)
            continue
        for b in range(2):

            @pl.when(y_lo != b)
            def _():
                issue(z_first(k, b))

    for n in range(3):
        gathered(n, 2)
    for far in range(2):
        product(far, 2, 2, last=3)
    lax.fori_loop(2, CHUNKS + 3, step, 0)
    arrived(landed, sem_b.at[0])

    lax.fori_loop(CHUNKS + 3, CHUNKS + LAG, step, 0)

    all_sent = (
        xs.at[0, 0, pl.ds(0, 6)], xs.at[0, pl.ds(0, 2)], xs.at[0, 0], xs.at[0], zs.at[:, pl.ds(0, 6)],
        zs.at[pl.ds(0, 3), pl.ds(0, 3)], zs.at[pl.ds(0, 3), pl.ds(0, 3)], landed, yin, vs,
    )
    for n, ref in enumerate(all_sent):
        arrived(ref, sent.at[n])


def finish(order, gathered, summed, tiles, gram, sem_t, sem_g):
    for q in range(tiles.shape[0]):
        pltpu.make_async_copy(gathered.at[order[0, q]], tiles.at[q], sem_t).start()
    whole = pltpu.make_async_copy(summed, gram, sem_g)
    whole.start()
    pltpu.make_async_copy(gathered, tiles, sem_t).wait()
    whole.wait()


def per_device(snapshots, weights, next_bricks, brick_source):
    rows, width = snapshots.shape
    depth, own = rows // 4, 2 * width
    scale = 1.0 / math.sqrt(rows * lax.axis_size("rows"))
    f32, bf16, dma = jnp.float32, jnp.bfloat16, pltpu.SemaphoreType.DMA
    vmem = pltpu.VMEM
    space = lambda kind: pl.BlockSpec(memory_space=kind)
    count = rows // BRICK
    summed, landed = pl.pallas_call(
        functools.partial(kernel, scale),
        out_shape=(
            vmem((2 * width, width), f32),
            vmem((count, BRICK, width), f32),
        ),
        in_specs=[space(pl.ANY), space(pl.ANY), space(pl.ANY)],
        out_specs=(space(vmem), space(pl.ANY)),
        scratch_shapes=[
            vmem((1, rows), f32),
            vmem((2, 4, CHUNKS, depth, LANES), f32),
            vmem((own, 2 * depth), bf16),
            vmem((own, 2 * depth), bf16),
            vmem((2 * depth, 4 * LANES), bf16),
            vmem((2 * depth, 4 * LANES), bf16),
            vmem((CHUNKS, 4, own, LANES), f32),
            vmem((6, CHUNKS, own // 2, LANES), f32),
            vmem((CHUNKS // 2, 3, own // 2, LANES), f32),
            vmem((2, 2, next_bricks.shape[0] // BRICK, BRICK, width), f32),
            vmem((3, 2, next_bricks.shape[0] // BRICK, BRICK, width), f32),
            vmem((3, 4, own // 2, LANES), f32),
            vmem((6, own // 4, LANES), f32),
            dma((CHUNKS,)), dma((2, CHUNKS)), dma((CHUNKS,)), dma((4, CHUNKS)), dma((2, CHUNKS)), dma((4,)),
            dma((1,)), dma((2, 2)), dma((1,)), dma((1,)), dma((2,)), dma, dma((10,)),
        ],
        compiler_params=pltpu.CompilerParams(
            collective_id=0, has_side_effects=True, vmem_limit_bytes=62464 * 1024
        ),
    )(snapshots, weights.reshape(1, rows), next_bricks.reshape(-1, BRICK, next_bricks.shape[1]))
    tiles, gram = pl.pallas_call(
        finish,
        out_shape=(
            jax.ShapeDtypeStruct((count, BRICK, width), f32),
            jax.ShapeDtypeStruct((2 * width, width), f32),
        ),
        in_specs=[space(pltpu.SMEM), space(pl.ANY), space(pl.ANY)],
        out_specs=(space(pl.ANY), space(pl.ANY)),
        scratch_shapes=[dma, dma],
        compiler_params=pltpu.CompilerParams(vmem_limit_bytes=2 * 1024 * 1024),
    )(brick_source, landed, summed)
    return gram, tiles.reshape(rows, width)


def solution(mesh):
    return jax.shard_map(
        per_device,
        mesh=mesh,
        in_specs=(P("rows", "snaps"), P("rows"), P(("rows", "snaps"), None), P("rows", None)),
        out_specs=(P("rows", "snaps"), P("rows", "snaps")),
        check_vma=False,
    )
```

```python
import functools
import math

import jax
import jax.numpy as jnp
from jax import lax
from jax.experimental import pallas as pl
from jax.experimental.pallas import tpu as pltpu
from jax.sharding import PartitionSpec as P

BRICK = 32
NX, NZ = 4, 4
CHUNKS = 8
LANES = 128
LAG = 4
MESH = pl.DeviceIdType.MESH


def kernel(
    scale, snap, weights, bricks, gram, landed,
    w_ref, xs, ahi, alo, bhi, blo, ps, zs, ys, relay, across, yin, vs,
    sem_a, sem_x, sem_h, sem_s, sem_z, sem_y, sem_b, sem_r, sem_o, sem_v, sem_w, sem_c,
    sent,
):
    rb, me = lax.axis_index("rows"), lax.axis_index("snaps")
    z, y_hi = rb // 2, rb % 2
    x, y_lo, c = me // 4, (me // 2) % 2, me % 2
    y = y_hi * 2 + y_lo
    depth = xs.shape[3]
    half = depth // 2

    def snap_of(xx, yl, cc):
        return xx * 4 + yl * 2 + cc

    right = (rb, snap_of((x + 1) % NX, y_lo, c))
    left = (rb, snap_of((x + 3) % NX, y_lo, c))
    twin = (rb, snap_of(x, y_lo, 1 - c))
    up = (((z + 1) % NZ) * 2 + y_hi, me)
    down = (((z + 3) % NZ) * 2 + y_hi, me)

    def round_of(far, part, cc):
        if far == 0:
            return 3 + cc if part else 1 - cc
        return 6 + cc if part else 2 + 3 * cc

    def send(src, dst, s_sem, r_sem, to):
        return pltpu.make_async_remote_copy(
            src_ref=src, dst_ref=dst, send_sem=s_sem, recv_sem=r_sem, device_id=to, device_id_type=MESH
        )

    def arrived(dst, sem):
        pltpu.make_async_copy(dst, dst, sem).wait()

    def reshard(o, part):
        y2, c2 = (y_lo + o // 2) % 2, (c + o % 2) % 2
        q2 = y2 * 2 + c2
        k = round_of(o // 2, part, c)
        src = snap.at[pl.ds(pl.multiple_of(q2 * depth, depth), depth), pl.ds(part * LANES, LANES)]
        dst = xs.at[c2, 0, k]
        if o == 0:
            return pltpu.make_async_copy(src, dst, sem_a.at[k])
        to = (rb, snap_of(x, y2, c2))
        return send(src, dst, sent.at[0], sem_a.at[k], to)

    def brick(o):
        s2 = snap_of(x, (y_lo + o // 2) % 2, (c + o % 2) % 2)
        width = landed.shape[2]
        src = bricks.at[:, :, pl.ds(pl.multiple_of(s2 * width, LANES), width)]
        count = bricks.shape[0]
        dst = landed.at[pl.ds(me * count, count)]
        if o == 0:
            return pltpu.make_async_copy(src, dst, sem_b.at[0])
        return send(src, dst, sent.at[6], sem_b.at[0], (rb, s2))

    def brick_cols(dx, dy, dc):
        width = landed.shape[2]
        s2 = snap_of((x + dx) % NX, (y_lo + dy) % 2, (c + dc) % 2)
        return bricks.at[:, :, pl.ds(pl.multiple_of(s2 * width, LANES), width)]

    def rows_from(source):
        return landed.at[pl.ds(source * bricks.shape[0], bricks.shape[0])]

    def brick_over(dx, dc):
        to = (rb, snap_of(x, 1 - y_lo, c))
        dst = across.at[dx - 1, dc]
        return send(brick_cols(dx, 1, dc), dst, sent.at[6], sem_o.at[0], to)

    def held_bricks(dx, dy, dc):
        return across.at[dx - 1, dc] if dy else brick_cols(dx, 0, dc)

    def brick_near(dx, dy, dc):
        source = snap_of(x, (y_lo + dy) % 2, c)
        to = (rb, snap_of((x + dx) % NX, y_lo, (c + dc) % 2))
        sem = sent.at[7]
        return send(held_bricks(dx, dy, dc), rows_from(source), sem, sem_b.at[0], to)

    def brick_far(g, dy):
        ahead, behind = (x + 1 + 2 * g) % NX, (x + 3 - 2 * g) % NX
        source = snap_of(behind, (y_lo + dy) % 2, c)
        to = (rb, snap_of(ahead, y_lo, (c + g) % 2))
        hop = send(
            held_bricks(2, dy, g), relay.at[g, dy], sent.at[7], sem_r.at[g, dy], left if g else right
        )
        return hop, send(relay.at[g, dy], rows_from(source), sent.at[7], sem_b.at[0], to)

    near = [(dx, dy, dc) for dx in (1, 3) for dy in range(2) for dc in range(2)]
    over = [(dx, dc) for dx in (1, 2, 3) for dc in range(2)]

    w_copy = pltpu.make_async_copy(weights, w_ref, sem_c)
    w_copy.start()
    for part in range(2):
        reshard(0, part).start()
    brick(0).start()

    barrier = pltpu.get_barrier_semaphore()
    for o in range(1, 16):
        pl.semaphore_signal(barrier, inc=1, device_id=(rb, (me + o) % 16), device_id_type=MESH)
    pl.semaphore_signal(barrier, inc=1, device_id=up, device_id_type=MESH)
    pl.semaphore_signal(barrier, inc=1, device_id=down, device_id_type=MESH)
    for yl in range(2):
        far = (z * 2 + 1 - y_hi, snap_of(x, yl, c))
        pl.semaphore_signal(barrier, inc=1, device_id=far, device_id_type=MESH)
    pl.semaphore_wait(barrier, 19)

    for part in range(2):
        for o in (1, 2, 3):
            reshard(o, part).start()
    brick(1).start()

    def first_hop(k):
        return (
            send(xs.at[c, 0, k], xs.at[c, 3, k], sent.at[1], sem_x.at[k], right),
            send(xs.at[c, 0, k], xs.at[c, 1, k], sent.at[1], sem_x.at[k], left),
        )

    def first_share(k):
        return (send(xs.at[c, 0, k], xs.at[c, 0, k], sent.at[3], sem_s.at[0, k], twin),)

    def second_hop(k):
        lo_rows, hi_rows = pl.ds(0, half), pl.ds(half, half)
        return (
            send(xs.at[c, 3, k, lo_rows], xs.at[c, 2, k, lo_rows], sent.at[2], sem_h.at[k], right),
            send(xs.at[c, 1, k, hi_rows], xs.at[c, 2, k, hi_rows], sent.at[2], sem_h.at[k], left),
            send(xs.at[c, 3, k], xs.at[c, 3, k], sent.at[3], sem_s.at[3, k], twin),
            send(xs.at[c, 1, k], xs.at[c, 1, k], sent.at[3], sem_s.at[1, k], twin),
        )

    def last_share(k):
        return (send(xs.at[c, 2, k], xs.at[c, 2, k], sent.at[3], sem_s.at[2, k], twin),)

    own = ps.shape[2]
    top, bottom = pl.ds(0, own // 2), pl.ds(own // 2, own // 2)

    def slot_of(j):
        return (j - x + 2 * NX) % NX

    def z_send(n, k, j, rows, to):
        return send(ps.at[k, slot_of(j), rows], zs.at[n, k], sent.at[4], sem_z.at[min(n // 2, 1), k], to)

    def z_first(k, b):
        if b == 0:
            return (z_send(0, k, z + 2, top, down), z_send(2, k, z + 1, top, up))
        return (z_send(1, k, z + 2, bottom, up), z_send(3, k, z - 1, bottom, down))

    def z_second(k):
        return (z_send(4, k, z - 1, top, down), z_send(5, k, z + 1, bottom, up))

    def z_add(k, j, rows, ns):
        d = slot_of(j)
        total = ps[k, d, rows]
        for n in ns:
            total = total + zs[n, k]
        ps[k, d, rows] = total

    def y_send(b, k):
        far = k // 5
        h, m = (y_lo + far) % 2, (1 - far) * ((k + 2) // 2) + far * (k - 4)
        yr = h * 2 + b
        slot = (y - yr + 8) % 4 - 1
        rows = top if b == 0 else bottom
        to = (z * 2 + h, snap_of(x, b, c))
        return yr, send(ps.at[k, slot_of(z), rows], ys.at[m, slot], sent.at[5], sem_y.at[m], to)

    def y_first(k, b):
        h = (y_lo + k - 1) % 2
        yr = h * 2 + b
        slot = (y - yr + 8) % 4 - 1
        rows = top if b == 0 else bottom
        to = (z * 2 + h, snap_of(x, b, c))
        return yr, send(ps.at[k, :, rows], yin.at[slot], sent.at[8], sem_v.at[0], to)

    def y_first_go(k):
        for b in range(2):
            yr, copy = y_first(k, b)

            @pl.when(y != yr)
            def _():
                copy.start()

    mine = 1 + (y_hi + y_lo) % 2
    piece = own // 4

    def v_rows(part):
        return pl.ds(pl.multiple_of(y_lo * (own // 2) + part * piece, piece), piece)

    def v_send(n, j, part, to):
        return send(ps.at[mine, slot_of(j), v_rows(part)], vs.at[n], sent.at[9], sem_w.at[min(n // 2, 1)], to)

    def v_first():
        return (v_send(0, z + 2, 0, down), v_send(1, z + 2, 1, up), v_send(2, z + 1, 0, up), v_send(3, z - 1, 1, down))

    def v_second():
        return (v_send(4, z - 1, 0, down), v_send(5, z + 1, 1, up))

    def v_add(j, part, ns):
        d = slot_of(j)
        total = ps[mine, d, v_rows(part)]
        for n in ns:
            total = total + vs[n]
        ps[mine, d, v_rows(part)] = total

    def issue(copies):
        for copy in copies:
            copy.start()

    def own_operand(far):
        for part in range(2):
            k = round_of(far, part, c)
            at = ((y_lo + far) % 2) * 2 * LANES + part * LANES
            rows = pl.ds(pl.multiple_of(at, LANES), LANES)
            for s in range(2):
                w = w_ref[:, pl.ds(pl.multiple_of(y_lo * 2 * depth + s * depth, LANES), depth)]
                block = xs[s, 0, k].T * (w * scale)
                hi = block.astype(jnp.bfloat16)
                cols = pl.ds(s * depth, depth)
                ahi[rows, cols] = hi
                alo[rows, cols] = (block - hi.astype(jnp.float32)).astype(jnp.bfloat16)

    def split(d, k, at):
        for s in range(2):
            block = xs[s, d, k]
            hi = block.astype(jnp.bfloat16)
            rows, cols = pl.ds(s * depth, depth), pl.ds(at, LANES)
            bhi[rows, cols] = hi
            blo[rows, cols] = (block - hi.astype(jnp.float32)).astype(jnp.bfloat16)

    order_of = (0, 1, 3, 2)

    def product(far, k, k2, first=0, last=4):
        dot = functools.partial(jnp.dot, preferred_element_type=jnp.float32)
        size = own // 2
        rows = pl.ds(pl.multiple_of(((y_lo + far) % 2) * size, size), size)
        cols = pl.ds(first * LANES, (last - first) * LANES)
        a, b = ahi[rows, :], bhi[:, cols]
        out = dot(a, b) + (dot(a, blo[:, cols]) + dot(alo[rows, :], b))
        for n in range(first, last):
            d = order_of[n]
            ps[k2 if d == 2 else k, d, rows] = out[:, (n - first) * LANES : (n - first + 1) * LANES]

    def gathered(n, k):
        d = order_of[n]
        if d:
            arrived(xs.at[1 - c, d, k], sem_s.at[d, k])
        split(d, k, n * LANES)

    def z_go(k, late, direct):
        for b in range(2):
            j = z + 1 - 2 * b if direct else z + 2
            copy = z_first(k, b)[direct]

            @pl.when((slot_of(j) == 2) == late)
            def _():
                copy.start()

    def early(k):
        for n in range(4):
            gathered(n, k)
        product(0, k, k)
        for b in range(0 if k else 2):

            @pl.when(y_lo == b)
            def _():
                issue(z_first(k, b))

    def pass_on(k):
        arrived(xs.at[c, pl.ds(0, 2), k], sem_x.at[k])
        issue(second_hop(k))

    def pass_last(k):
        arrived(xs.at[c, 2, k], sem_h.at[k])
        issue(last_share(k))

    def step(i, carry):
        @pl.when(i + 1 < CHUNKS)
        def _():
            pass_on(i + 1)

        @pl.when(i + 3 < CHUNKS)
        def _():
            issue(first_hop(i + 3))

        @pl.when(i + 1 == CHUNKS - 1)
        def _():
            arrived(across, sem_o.at[0])
            for n in range(4):
                brick_far(n % 2, n // 2)[0].start()
            for at in near:
                brick_near(*at).start()

        @pl.when(i < CHUNKS)
        def _():
            pass_last(i)

        def z_pass(k):
            arrived(zs.at[pl.ds(0, 2), k], sem_z.at[0, k])
            z_add(k, z - 1, top, (0,))
            z_add(k, z + 1, bottom, (1,))
            issue(z_second(k))

        def z_last(k):
            arrived(zs.at[pl.ds(2, 4), k], sem_z.at[1, k])
            z_add(k, z, top, (2, 4))
            z_add(k, z, bottom, (3, 5))
            for b in range(2):
                yr, copy = y_send(b, k)

                @pl.when(y != yr)
                def _():
                    copy.start()

        @pl.when((i >= 4) & (i <= 6))
        def _():
            z_pass(i - 1)

        @pl.when(i + 1 < CHUNKS)
        def _():
            for n in range(3):
                gathered(n, i + 1)
            gathered(3, i)
            for far in range(2):
                product(far, i + 1, i)
            @pl.when(i == 2)
            def _():
                y_first_go(2)

            @pl.when(i > 2)
            def _():
                z_go(i, True, 0)

            z_go(i + 1, False, 0)

            @pl.when(i > 2)
            def _():
                z_go(i, True, 1)

            @pl.when(i + 1 < CHUNKS - 1)
            def _():
                z_go(i + 1, False, 1)

        @pl.when(i == CHUNKS - 1)
        def _():
            gathered(3, i)
            for far in range(2):
                product(far, i, i, first=3)
            z_go(i, True, 0)
            z_pass(i - 1)
            for b in range(2):
                z_first(i, b)[1].start()

        @pl.when(i == 2)
        def _():
            z_pass(0)

        @pl.when(i == CHUNKS)
        def _():
            z_pass(i - 1)

        @pl.when(i == 8)
        def _():
            arrived(yin, sem_v.at[0])
            rows = pl.ds(pl.multiple_of(y_lo * (own // 2), own // 2), own // 2)
            for d in range(4):
                ps[mine, d, rows] = ps[mine, d, rows] + (yin[0, d] + (yin[1, d] + yin[2, d]))
            issue(v_first())

        @pl.when(i == 4)
        def _():
            z_last(0)

        @pl.when((i >= 6) & (i < CHUNKS + 3))
        def _():
            z_last(i - 3)

        @pl.when(i == CHUNKS - 1)
        def _():
            for n in range(4):
                g, dy = n // 2, n % 2
                arrived(relay.at[g, dy], sem_r.at[g, dy])
                brick_far(g, dy)[1].start()

        @pl.when(i == 10)
        def _():
            arrived(vs.at[pl.ds(0, 2)], sem_w.at[0])
            v_add(z - 1, 0, (0,))
            v_add(z + 1, 1, (1,))
            issue(v_second())

        @pl.when(i == 11)
        def _():
            arrived(vs.at[pl.ds(2, 4)], sem_w.at[1])
            v_add(z, 0, (2, 4))
            v_add(z, 1, (3, 5))
            rows = pl.ds(pl.multiple_of(y_lo * (own // 2), own // 2), own // 2)
            gram[pl.ds(0, LANES), :] = ps[mine, slot_of(z), rows].T

        @pl.when(i >= 5 + LAG)
        def _():
            m = i - 4 - LAG
            far = (y_hi + y_lo) % 2
            k = (1 - far) * (m + m // 2 - (3 - m) // 2) + far * (m + 4)
            arrived(ys.at[m], sem_y.at[m])
            here = ps[k, slot_of(z), pl.ds(pl.multiple_of(y_lo * (own // 2), own // 2), own // 2)]
            total = here + (ys[m, 0] + (ys[m, 1] + ys[m, 2]))
            at = (m % 2) * 2 * LANES + (m // 2) * LANES
            gram[pl.ds(pl.multiple_of(at, LANES), LANES), :] = total.T

        return carry

    def ready(k):
        arrived(xs.at[c, 0, k], sem_a.at[k])
        issue(first_share(k))

    for k in (0, 1, 3, 4):
        ready(k)
        if k < 2:
            issue(first_hop(k))
    for k in (0, 1, 3, 4):
        arrived(xs.at[1 - c, 0, k], sem_s.at[0, k])
    w_copy.wait()
    own_operand(0)
    pass_on(0)
    ready(2)
    issue(first_hop(2))
    pass_on(1)
    issue(first_hop(3))
    pass_last(0)
    ready(5)
    early(0)
    pass_on(2)
    issue(first_hop(4))
    pass_last(1)
    ready(6)
    ready(7)
    early(1)
    brick(2).start()
    brick(3).start()
    for at in over:
        brick_over(*at).start()
    for k in (2, 5, 6, 7):
        arrived(xs.at[1 - c, 0, k], sem_s.at[0, k])
    own_operand(1)
    for k in range(2):
        for n in range(4):
            split(order_of[n], k, n * LANES)
        product(1, k, k)
        if k == 1:
            y_first_go(1)
            continue
        for b in range(2):

            @pl.when(y_lo != b)
            def _():
                issue(z_first(k, b))

    for n in range(3):
        gathered(n, 2)
    for far in range(2):
        product(far, 2, 2, last=3)
    lax.fori_loop(2, CHUNKS + 3, step, 0)
    arrived(landed, sem_b.at[0])

    lax.fori_loop(CHUNKS + 3, CHUNKS + LAG, step, 0)

    all_sent = (
        xs.at[0, 0, pl.ds(0, 6)], xs.at[0, pl.ds(0, 2)], xs.at[0, 0], xs.at[0], zs.at[:, pl.ds(0, 6)],
        zs.at[pl.ds(0, 3), pl.ds(0, 3)], zs.at[pl.ds(0, 3), pl.ds(0, 3)], landed, yin, vs,
    )
    for n, ref in enumerate(all_sent):
        arrived(ref, sent.at[n])


def finish(order, gathered, summed, tiles, gram, sem_t, sem_g):
    whole = pltpu.make_async_copy(summed, gram, sem_g)
    whole.start()
    for q in range(tiles.shape[0]):
        pltpu.make_async_copy(gathered.at[order[0, q]], tiles.at[q], sem_t).start()
    pltpu.make_async_copy(gathered, tiles, sem_t).wait()
    whole.wait()


def per_device(snapshots, weights, next_bricks, brick_source):
    rows, width = snapshots.shape
    depth, own = rows // 4, 2 * width
    scale = 1.0 / math.sqrt(rows * lax.axis_size("rows"))
    f32, bf16, dma = jnp.float32, jnp.bfloat16, pltpu.SemaphoreType.DMA
    vmem = pltpu.VMEM
    space = lambda kind: pl.BlockSpec(memory_space=kind)
    count = rows // BRICK
    summed, landed = pl.pallas_call(
        functools.partial(kernel, scale),
        out_shape=(
            vmem((2 * width, width), f32),
            vmem((count, BRICK, width), f32),
        ),
        in_specs=[space(pl.ANY), space(pl.ANY), space(pl.ANY)],
        out_specs=(space(vmem), space(pl.ANY)),
        scratch_shapes=[
            vmem((1, rows), f32),
            vmem((2, 4, CHUNKS, depth, LANES), f32),
            vmem((own, 2 * depth), bf16),
            vmem((own, 2 * depth), bf16),
            vmem((2 * depth, 4 * LANES), bf16),
            vmem((2 * depth, 4 * LANES), bf16),
            vmem((CHUNKS, 4, own, LANES), f32),
            vmem((6, CHUNKS, own // 2, LANES), f32),
            vmem((CHUNKS // 2, 3, own // 2, LANES), f32),
            vmem((2, 2, next_bricks.shape[0] // BRICK, BRICK, width), f32),
            vmem((3, 2, next_bricks.shape[0] // BRICK, BRICK, width), f32),
            vmem((3, 4, own // 2, LANES), f32),
            vmem((6, own // 4, LANES), f32),
            dma((CHUNKS,)), dma((CHUNKS,)), dma((CHUNKS,)), dma((4, CHUNKS)), dma((2, CHUNKS)), dma((4,)),
            dma((1,)), dma((2, 2)), dma((1,)), dma((1,)), dma((2,)), dma, dma((10,)),
        ],
        compiler_params=pltpu.CompilerParams(
            collective_id=0, has_side_effects=True, vmem_limit_bytes=62464 * 1024
        ),
    )(snapshots, weights.reshape(1, rows), next_bricks.reshape(-1, BRICK, next_bricks.shape[1]))
    tiles, gram = pl.pallas_call(
        finish,
        out_shape=(
            jax.ShapeDtypeStruct((count, BRICK, width), f32),
            jax.ShapeDtypeStruct((2 * width, width), f32),
        ),
        in_specs=[space(pltpu.SMEM), space(pl.ANY), space(pl.ANY)],
        out_specs=(space(pl.ANY), space(pl.ANY)),
        scratch_shapes=[dma, dma],
        compiler_params=pltpu.CompilerParams(vmem_limit_bytes=2 * 1024 * 1024),
    )(brick_source, landed, summed)
    return gram, tiles.reshape(rows, width)


def solution(mesh):
    return jax.shard_map(
        per_device,
        mesh=mesh,
        in_specs=(P("rows", "snaps"), P("rows"), P(("rows", "snaps"), None), P("rows", None)),
        out_specs=(P("rows", "snaps"), P("rows", "snaps")),
        check_vma=False,
    )
```
